256 devices in a mesh: dp: 32 (over y, x, z_lo), mp: 8 (over z_hi, core).
Axes of the slice: x: 4, y: 4, z: 8 (z_hi: 4, z_lo: 2; z = z_hi * 2 + z_lo), core: 2. Of those that a mesh axis runs over, the one named last changes fastest.
Arguments:
- hidden: bfloat16 [65536, 13824], P('dp', 'mp'), may hold values from -6 to 6
- out_grad: bfloat16 [65536, 5120], P('dp', 'mp'), may hold values from -6 to 6
- proj_in: bfloat16 [64, 13824], P(None, 'mp'), may hold values from -0.0546875 to 0.0546875
- proj_out: bfloat16 [64, 5120], P(None, 'mp'), may hold values from -0.078125 to 0.078125
- segment_ids: int32 [32, 2048], P('dp'), may hold values from 0 to 15, never falling along the last dimension, each value on 1 to 1024 neighbouring positions
Outputs:
- features: float32 [512, 4096], P('dp')
- gram: float32 [4096, 4096], P(('dp', 'mp'))
The draws below stay inside these ranges and needn't reach their ends.
Inputs may be any that keep to these rules, and one draw needn't show every extreme that they name: `segment_ids`: within each row the numbers never fall; each of the 16 numbers names 1 to 1024 tokens of the row.
All inputs are finite; a program needn't handle non-finite values.
Results may differ from the reference program's by a relative error of at most 0.0003.
Values sent between devices are 32-bit elements; how exact they have to be, the bound alone decides.
A program may use at most 64 MiB of HBM per device.

```python
import math
import jax
import jax.numpy as jnp
import numpy as np
from jax import lax

D = 5120
FF = 13824
RANK = 64
TOK_DEV = 2048
EX_DEV = 16
PROJ = 4096
TOKENS = 65536
EXAMPLES = 512
N_DP = 32


def block_scale(rng, extent, pieces, least, largest):
    def one(dim, parts):
        heights = jax.random.uniform(jax.random.fold_in(jax.random.fold_in(rng, 6), dim), (parts,), jnp.float32, least / len(pieces), largest / len(pieces))
        return jnp.repeat(jnp.exp(heights), extent[dim] // parts).reshape((-1,) + (1,) * (len(extent) - dim - 1))

    level = one(*pieces[0])
    for cut in pieces[1:]:
        level = level * one(*cut)
    return level


def split_up(count, total, bound, lean):
    loads = [(1 << 20) // math.isqrt(rank ** lean) + 1 for rank in range(2, count + 1)]
    spare, given = total - bound - (count - 1), [1] * (count - 1)
    while spare > 0:
        movable = [i for i in range(count - 1) if given[i] < bound]
        pool, remaining = sum([loads[i] for i in movable]), spare
        for i in movable:
            addition = min(bound - given[i], max(1, remaining * loads[i] // pool), spare)
            given[i] = given[i] + addition
            spare = spare - addition
    return np.array([bound] + given)


def ragged(rng, amount, total, limit, slope):
    if amount == 2:
        one = jax.random.randint(rng, (), max(1, total - limit), min(limit, total - 1) + 1)
        return jnp.stack([one, total - one])
    sizes = jnp.asarray(split_up(amount, total, limit, slope), jnp.int32)
    pairs = (amount - 1) // 2
    source_of, receiver = sizes[1:1 + 2 * pairs:2], sizes[2:2 + 2 * pairs:2]
    slack = jnp.minimum(source_of - 1, limit - receiver)
    passed = jax.random.randint(jax.random.fold_in(rng, 1), (pairs,), 0, 1 << 20) % (slack + 1)
    sizes = sizes.at[1:1 + 2 * pairs:2].set(source_of - passed).at[2:2 + 2 * pairs:2].set(receiver + passed)
    return sizes[jax.random.permutation(jax.random.fold_in(rng, 2), amount)]


def noise(rng, shape, width, most, pieces=(), held_as=jnp.bfloat16):
    loudness = block_scale(rng, shape, pieces, -0.22, 0.18) if pieces else 1.0
    entries = jax.random.normal(rng, shape, jnp.float32) * width * loudness
    return jnp.minimum(jnp.maximum(entries, -most), most).astype(held_as)


def setup_inputs(seed: int = 0) -> dict:
    key_list = jax.random.split(jax.random.key(seed), 6)
    hidden = noise(key_list[0], (TOKENS, FF), 1.0, 6.0, ((0, 32), (1, 8)))
    out_grad = noise(key_list[1], (TOKENS, D), 1.0, 6.0, ((0, 32), (1, 8)))
    proj_in = noise(key_list[2], (RANK, FF), FF ** -0.5, 0.0546875, ((1, 8),))
    proj_out = noise(key_list[3], (RANK, D), D ** -0.5, 0.078125, ((1, 8),))
    segment_ids = jax.vmap(lambda own: jnp.searchsorted(jnp.cumsum(ragged(own, EX_DEV, TOK_DEV, TOK_DEV // 2, 2)), jnp.arange(TOK_DEV), side="right"))(jax.random.split(key_list[4], N_DP)).reshape((N_DP, TOK_DEV)).astype(jnp.int32)
    return dict(hidden=hidden, out_grad=out_grad, proj_in=proj_in, proj_out=proj_out, segment_ids=segment_ids)


def example_grads(example_ids, inputs, outputs, examples):
    onehot = (example_ids[None, :] == jnp.arange(examples, dtype=jnp.int32)[:, None]).astype(jnp.float32)
    counts = lax.optimization_barrier(jnp.sum(onehot, axis=1))
    weighted = onehot[:, :, None] * outputs[None, :, :]
    grads = jnp.einsum('eti,tj->eij', weighted, inputs, precision=lax.Precision.HIGHEST)
    return grads.reshape(examples, -1) / jnp.sqrt(counts)[:, None]

def reference(hidden, out_grad, proj_in, proj_out, segment_ids):
    hidden_rows = hidden.reshape(N_DP, TOK_DEV, FF)
    grad_rows = out_grad.reshape(N_DP, TOK_DEV, D)

    def per_sequence(operands):
        hidden_row, grad_row, ids_row = operands
        inputs = lax.dot_general(hidden_row, proj_in, (((1,), (1,)), ((), ())), preferred_element_type=jnp.float32)
        outputs = lax.dot_general(grad_row, proj_out, (((1,), (1,)), ((), ())), preferred_element_type=jnp.float32)
        return example_grads(ids_row, inputs, outputs, EX_DEV)
    features = lax.map(per_sequence, (hidden_rows, grad_rows, segment_ids)).reshape(EXAMPLES, PROJ)
    gram = lax.dot_general(features, features, (((0,), (0,)), ((), ())), precision=lax.Precision.HIGHEST, preferred_element_type=jnp.float32) / EXAMPLES
    return (features, gram)
```

```python
import jax
import jax.numpy as jnp
from jax import lax
from jax.experimental import pallas as pl
from jax.experimental.pallas import tpu as pltpu
from jax.sharding import PartitionSpec as P

MESH = pl.DeviceIdType.MESH
EX = 16
DP = 32
MP = 8
F32 = jnp.float32
BF16 = jnp.bfloat16


def split(x):
    hi = x.astype(BF16)
    return hi, (x - hi.astype(F32)).astype(BF16)


def dot_nt(a, b):
    return lax.dot_general(a, b, (((1,), (1,)), ((), ())), preferred_element_type=F32)


def dot(a, b):
    return lax.dot_general(a, b, (((1,), (0,)), ((), ())), preferred_element_type=F32)


def kernel(
    hid,
    og,
    pin,
    pout,
    seg,
    feat_o,
    gram_o,
    hbuf,
    gbuf,
    wh,
    wg,
    psend,
    pmine,
    precv,
    zrecv,
    zrel,
    pown,
    ppart,
    whi,
    wlo,
    rb,
    gbuf2,
    brecv,
    fown,
    fpar,
    fparp,
    cc,
    rr,
    rrp,
    gb,
    gg,
    lsem,
    d2d_s,
    d2d_r,
    z_s,
    z_r,
    px_s,
    px_r,
    b_s,
    b_r,
    c1_s,
    c1_r,
    c2_s,
    c2_r,
    c3_s,
    c3_r,
    c4_s,
    c4_r,
    ft_s,
    ft_r,
    dd_s,
    dd_r,
):
    dp = lax.axis_index("dp")
    m = lax.axis_index("mp")
    c = m // 2
    h = m % 2
    p = dp // 2
    zl = dp % 2
    partner = c * 2 + (1 - h)
    nblk = 256

    def rc(src, dst, ss, rs, tdp, tmp):
        return pltpu.make_async_remote_copy(
            src_ref=src,
            dst_ref=dst,
            send_sem=ss,
            recv_sem=rs,
            device_id=(tdp, tmp),
            device_id_type=MESH,
        )

    owners = [(c + 2) % 4, (c + 1) % 4, (c + 3) % 4, c]
    blocks = []
    for o in owners:
        blocks.append(o * 2 + (1 - h))
        blocks.append(o * 2 + h)
    loads = []
    for k, blk in enumerate(blocks):
        rows = pl.ds(pl.multiple_of(blk * nblk, nblk), nblk)
        a = pltpu.make_async_copy(hid.at[rows], hbuf.at[k], lsem.at[2 * k])
        b = pltpu.make_async_copy(og.at[rows], gbuf.at[k], lsem.at[2 * k + 1])
        a.start()
        b.start()
        loads.append((a, b))

    barrier = pltpu.get_barrier_semaphore()

    def greet_dp(k, carry):
        pl.semaphore_signal(barrier, inc=1, device_id=((dp + k) % DP, m), device_id_type=MESH)
        return carry

    lax.fori_loop(1, DP, greet_dp, 0)

    def greet_own(k, carry):
        pl.semaphore_signal(barrier, inc=1, device_id=(dp, (m + k) % MP), device_id_type=MESH)
        pl.semaphore_signal(
            barrier, inc=1, device_id=(2 * p + (1 - zl), (m + k) % MP), device_id_type=MESH
        )
        return carry

    lax.fori_loop(1, MP, greet_own, 0)

    wh[0:64, :] = pin[...]
    wh[64:128, :] = jnp.zeros((64, wh.shape[1]), BF16)
    wg[0:64, :] = jnp.zeros((64, wg.shape[1]), BF16)
    wg[64:128, :] = pout[...]

    segv = seg[...]
    erow = lax.broadcasted_iota(jnp.int32, (EX, segv.shape[1]), 0)
    counts = jnp.sum(jnp.where(erow == segv, 1.0, 0.0).astype(F32), axis=1, keepdims=True)
    scale = 1.0 / jnp.sqrt(counts)

    def project(k):
        loads[k][0].wait()
        loads[k][1].wait()
        return dot_nt(hbuf[k], wh[...]) + dot_nt(gbuf[k], wg[...])

    d2d = []
    zsend = []
    up = (c + 1) % 4
    down = (c + 3) % 4

    def zcopy(k, src, to):
        return rc(src, zrecv.at[k], z_s.at[k], z_r.at[k], dp, to * 2 + h)

    def finish(k):
        d2d[k].wait_recv()
        pmine[k] = pmine[k] + precv[k]
        if k == 0:
            zsend.append(zcopy(0, pmine.at[0, 0:128], down))
            zsend.append(zcopy(1, pmine.at[0, 128:256], up))
            zsend[0].start()
            zsend[1].start()
        if k == 1:
            zsend.append(zcopy(2, pmine.at[1, 0:128], up))
            zsend[2].start()
        if k == 2:
            zsend.append(zcopy(3, pmine.at[2, 128:256], down))
            zsend[3].start()

    for k in range(4):
        psend[k] = project(2 * k)
        if k == 0:
            pl.semaphore_wait(barrier, DP - 1 + 2 * (MP - 1))
        d2d.append(rc(psend.at[k], precv.at[k], d2d_s.at[k], d2d_r.at[k], dp, partner))
        d2d[k].start()
        pmine[k] = project(2 * k + 1)
        if k >= 1:
            finish(k - 1)
    finish(3)

    zsend[0].wait_recv()
    zrel[0] = zrecv[0] + pmine[2, 0:128]
    zsend.append(zcopy(4, zrel.at[0], down))
    zsend[4].start()
    zsend[1].wait_recv()
    zrel[1] = zrecv[1] + pmine[1, 128:256]
    zsend.append(zcopy(5, zrel.at[1], up))
    zsend[5].start()
    zsend[2].wait_recv()
    zsend[3].wait_recv()
    zsend[4].wait_recv()
    zsend[5].wait_recv()
    pown[0:128] = pmine[3, 0:128] + zrecv[2] + zrecv[4]
    pown[128:256] = pmine[3, 128:256] + zrecv[3] + zrecv[5]

    px = rc(pown, ppart, px_s, px_r, dp, partner)
    px.start()

    def weigh(s, toks, blk):
        low = jnp.where(lax.broadcasted_iota(jnp.int32, (nblk, 128), 1) < 64, toks, 0.0)
        high = pltpu.roll(low, 64, 1)
        lh, ll = split(low)
        hh, hl = split(high)
        base = s * 512
        rb[base : base + 256, 0:128] = lh
        rb[base : base + 256, 128:256] = ll
        rb[base + 256 : base + 512, 0:128] = hh
        rb[base + 256 : base + 512, 128:256] = hl
        trans = toks.T
        ids = seg[:, pl.ds(pl.multiple_of(blk * nblk, nblk), nblk)]
        mask = lax.broadcasted_iota(jnp.int32, (EX, nblk), 0) == ids
        for cq in range(4):
            rows = jnp.where(h == 0, trans[64 + 16 * cq : 72 + 16 * cq], trans[72 + 16 * cq : 80 + 16 * cq])
            for k in range(4):
                tile = (cq * 2 + k % 2) * 2 + k // 2
                for par in range(2):
                    one = jnp.where(mask, rows[2 * k + par : 2 * k + par + 1, :], 0.0)
                    oh, ol = split(one)
                    whi[tile * 16 : tile * 16 + 16, base + par * 256 : base + par * 256 + 256] = oh
                    wlo[tile * 16 : tile * 16 + 16, base + par * 256 : base + par * 256 + 256] = ol

    def grads(s):
        cols = slice(s * 512, s * 512 + 512)
        both = dot(whi[:, cols], rb[cols, :])
        return both[:, 0:128] + both[:, 128:256] + dot(wlo[:, cols], rb[cols, 0:128])

    weigh(0, pown[...], m)
    g0 = grads(0)
    px.wait_recv()
    weigh(1, ppart[...], partner)
    gbuf2[...] = (g0 + grads(1)).reshape(4, 2, 2, 16, 128)

    bs = []
    for k in (2, 1, 3):
        to = (c + k) % 4
        cp = rc(gbuf2.at[to], brecv.at[k - 1], b_s.at[k - 1], b_r.at[k - 1], dp, to * 2 + h)
        cp.start()
        bs.append(cp)
    for cp in bs:
        cp.wait_recv()
    fown[...] = (gbuf2[c] + brecv[0] + brecv[1] + brecv[2]) * scale[None, None]

    def c2(k):
        to = (m + k) % MP
        return rc(fown.at[to % 2], fpar.at[m], c2_s.at[k], c2_r.at[k], dp, to)

    def c1(k):
        to = (dp + k) % DP
        return rc(fown.at[to % 2], cc.at[dp], c1_s.at[k], c1_r.at[k], to, m)

    def c3(k):
        to = (dp + k) % DP
        tp = to // 2
        return rc(fpar.at[tp // 2, tp % 2], rr.at[dp], c3_s.at[k], c3_r.at[k], to, m)

    for k in range(1, MP):
        c2(k).start()
    lax.fori_loop(1, DP, lambda k, v: (c1(k).start(), v)[1], 0)
    cc[dp] = fown[zl]
    fpar[m] = fown[h]
    for k in range(1, MP):
        c2(k).wait_recv()
    lax.fori_loop(1, DP, lambda k, v: (c3(k).start(), v)[1], 0)
    rr[dp] = fpar[p // 2, p % 2]
    ft = rc(fpar, fparp, ft_s, ft_r, dp, partner)
    ft.start()
    lax.fori_loop(1, DP, lambda k, v: (c3(k).wait_recv(), v)[1], 0)
    c4 = rc(rr, rrp, c4_s, c4_r, dp, partner)
    c4.start()
    ft.wait_recv()
    for q in range(MP):
        for k2 in range(2):
            col = 4 * q + 2 * k2
            feat_o[:, pl.ds(pl.multiple_of((col + h) * 128, 128), 128)] = fpar[q, k2]
            feat_o[:, pl.ds(pl.multiple_of((col + 1 - h) * 128, 128), 128)] = fparp[q, k2]
    lax.fori_loop(1, DP, lambda k, v: (c1(k).wait_recv(), v)[1], 0)

    cols = [cc[:, k2].reshape(DP * EX, 128) for k2 in range(2)]
    parts = [split(x) for x in cols]
    right = jnp.concatenate([parts[0][0], parts[1][0], parts[0][1], parts[1][1]], axis=1)

    def block(rows, par):
        lh, ll = split(rows[...].reshape(DP * EX, 128).T)
        both = dot(lh, right)
        res = both[:, 0:256] + both[:, 256:512] + dot(ll, right[:, 0:256])
        res = res * (1.0 / (DP * EX))
        for k2 in range(2):
            gb[par, :, k2] = res[:, k2 * 128 : k2 * 128 + 128].reshape(MP, 16, 128)

    block(rr, h)
    c4.wait_recv()
    block(rrp, 1 - h)

    me = zl * MP + m

    def dd(k):
        f = (me + k) % (2 * MP)
        return rc(gb.at[f // MP, f % MP], gg.at[me], dd_s.at[k], dd_r.at[k], 2 * p + f // MP, f % MP)

    for k in range(1, 2 * MP):
        dd(k).start()
    gg[me] = gb[zl, m]
    for k in range(1, 2 * MP):
        dd(k).wait_recv()
    for s in range(2 * MP):
        for k2 in range(2):
            i2 = 4 * (s % MP) + 2 * k2 + s // MP
            gram_o[:, i2 * 128 : i2 * 128 + 128] = gg[s, k2]

    for k in range(4):
        d2d[k].wait_send()
    for cp in zsend:
        cp.wait_send()
    px.wait_send()
    for cp in bs:
        cp.wait_send()
    for k in range(1, MP):
        c2(k).wait_send()
    lax.fori_loop(1, DP, lambda k, v: (c1(k).wait_send(), v)[1], 0)
    lax.fori_loop(1, DP, lambda k, v: (c3(k).wait_send(), v)[1], 0)
    c4.wait_send()
    ft.wait_send()
    for k in range(1, 2 * MP):
        dd(k).wait_send()


def body(hidden, out_grad, proj_in, proj_out, segment_ids):
    kin = hidden.shape[1]
    kout = out_grad.shape[1]
    vmem = pl.BlockSpec(memory_space=pltpu.VMEM)
    hbm = pl.BlockSpec(memory_space=pl.ANY)
    dma = pltpu.SemaphoreType.DMA
    scratch = [
        pltpu.VMEM((8, 256, kin), BF16),
        pltpu.VMEM((8, 256, kout), BF16),
        pltpu.VMEM((128, kin), BF16),
        pltpu.VMEM((128, kout), BF16),
        pltpu.VMEM((4, 256, 128), F32),
        pltpu.VMEM((4, 256, 128), F32),
        pltpu.VMEM((4, 256, 128), F32),
        pltpu.VMEM((6, 128, 128), F32),
        pltpu.VMEM((2, 128, 128), F32),
        pltpu.VMEM((256, 128), F32),
        pltpu.VMEM((256, 128), F32),
        pltpu.VMEM((256, 1024), BF16),
        pltpu.VMEM((256, 1024), BF16),
        pltpu.VMEM((1024, 256), BF16),
        pltpu.VMEM((4, 2, 2, 16, 128), F32),
        pltpu.VMEM((3, 2, 2, 16, 128), F32),
        pltpu.VMEM((2, 2, 16, 128), F32),
        pltpu.VMEM((8, 2, 16, 128), F32),
        pltpu.VMEM((8, 2, 16, 128), F32),
        pltpu.VMEM((32, 2, 16, 128), F32),
        pltpu.VMEM((32, 16, 128), F32),
        pltpu.VMEM((32, 16, 128), F32),
        pltpu.VMEM((2, 8, 2, 16, 128), F32),
        pltpu.VMEM((16, 2, 16, 128), F32),
        dma((16,)),
        dma((4,)),
        dma((4,)),
        dma((6,)),
        dma((6,)),
        dma,
        dma,
        dma((3,)),
        dma((3,)),
        dma((32,)),
        dma((32,)),
        dma((8,)),
        dma((8,)),
        dma((32,)),
        dma((32,)),
        dma,
        dma,
        dma,
        dma,
        dma((16,)),
        dma((16,)),
    ]
    return pl.pallas_call(
        kernel,
        out_shape=(
            jax.ShapeDtypeStruct((EX, 4096), F32),
            jax.ShapeDtypeStruct((16, 4096), F32),
        ),
        in_specs=[hbm, hbm, vmem, vmem, vmem],
        out_specs=(vmem, vmem),
        scratch_shapes=scratch,
        compiler_params=pltpu.CompilerParams(
            collective_id=0, has_side_effects=True, vmem_limit_bytes=40 << 20
        ),
        name="projected_gram",
    )(hidden, out_grad, proj_in, proj_out, segment_ids)


def solution(mesh):
    placed = (P("dp", "mp"), P("dp", "mp"), P(None, "mp"), P(None, "mp"), P("dp", None))
    return jax.shard_map(
        body,
        mesh=mesh,
        in_specs=placed,
        out_specs=(P("dp", None), P(("dp", "mp"), None)),
        check_vma=False,
    )
```

```python
import jax
import jax.numpy as jnp
from jax import lax
from jax.experimental import pallas as pl
from jax.experimental.pallas import tpu as pltpu
from jax.sharding import PartitionSpec as P

MESH = pl.DeviceIdType.MESH
EX = 16
DP = 32
MP = 8
F32 = jnp.float32
BF16 = jnp.bfloat16


def split(x):
    hi = x.astype(BF16)
    return hi, (x - hi.astype(F32)).astype(BF16)


def dot_nt(a, b):
    return lax.dot_general(a, b, (((1,), (1,)), ((), ())), preferred_element_type=F32)


def dot(a, b):
    return lax.dot_general(a, b, (((1,), (0,)), ((), ())), preferred_element_type=F32)


def kernel(
    hid,
    og,
    pin_h,
    pout_h,
    seg_h,
    feat_o,
    gram_o,
    pin,
    pout,
    seg,
    hbuf,
    gbuf,
    psend,
    pmine,
    precv,
    zrecv,
    zrel,
    pown,
    ppart,
    whi,
    wlo,
    rb,
    gbuf2,
    brecv,
    fown,
    fpar,
    fparp,
    cc,
    rr,
    rrp,
    gb,
    gg,
    lsem,
    d2d_s,
    d2d_r,
    z_s,
    z_r,
    px_s,
    px_r,
    b_s,
    b_r,
    c1_s,
    c1_r,
    c2_s,
    c2_r,
    c3_s,
    c3_r,
    c4_s,
    c4_r,
    ft_s,
    ft_r,
    dd_s,
    dd_r,
):
    dp = lax.axis_index("dp")
    m = lax.axis_index("mp")
    c = m // 2
    h = m % 2
    p = dp // 2
    zl = dp % 2
    partner = c * 2 + (1 - h)
    nblk = 256

    def rc(src, dst, ss, rs, tdp, tmp):
        return pltpu.make_async_remote_copy(
            src_ref=src,
            dst_ref=dst,
            send_sem=ss,
            recv_sem=rs,
            device_id=(tdp, tmp),
            device_id_type=MESH,
        )

    sent = []

    def drain():
        for wait in sent:
            wait()

    def launch(copy):
        copy.start()
        sent.append(copy.wait_send)

    def launch_each(n, f):
        each(n, lambda k: f(k).start())
        sent.append(lambda: each(n, lambda k: f(k).wait_send()))

    def each(n, f):
        lax.fori_loop(1, n, lambda k, v: (f(k), v)[1], 0)

    owners = [(c + 2) % 4, (c + 1) % 4, (c + 3) % 4, c]
    blocks = []
    for o in owners:
        blocks.append(o * 2 + (1 - h))
        blocks.append(o * 2 + h)
    small = []
    for k, (src, dst) in enumerate(((pin_h, pin), (pout_h, pout), (seg_h, seg))):
        small.append(pltpu.make_async_copy(src, dst, lsem.at[16 + k]))
        small[k].start()
    loads = []
    for k, blk in enumerate(blocks):
        rows = pl.ds(pl.multiple_of(blk * nblk, nblk), nblk)
        a = pltpu.make_async_copy(hid.at[:, rows], hbuf.at[k], lsem.at[2 * k])
        b = pltpu.make_async_copy(og.at[rows], gbuf.at[k], lsem.at[2 * k + 1])
        a.start()
        b.start()
        loads.append((a, b))

    barrier = pltpu.get_barrier_semaphore()

    def greet_dp(k, carry):
        pl.semaphore_signal(barrier, inc=1, device_id=((dp + k) % DP, m), device_id_type=MESH)
        return carry

    lax.fori_loop(1, DP, greet_dp, 0)

    def greet_own(k, carry):
        pl.semaphore_signal(barrier, inc=1, device_id=(dp, (m + k) % MP), device_id_type=MESH)
        pl.semaphore_signal(
            barrier, inc=1, device_id=(2 * p + (1 - zl), (m + k) % MP), device_id_type=MESH
        )
        return carry

    lax.fori_loop(1, MP, greet_own, 0)

    rb[...] = jnp.zeros(rb.shape, BF16)

    small[2].wait()
    segv = seg[...]
    erow = lax.broadcasted_iota(jnp.int32, (EX, segv.shape[1]), 0)
    counts = jnp.sum(jnp.where(erow == segv, 1.0, 0.0).astype(F32), axis=1, keepdims=True)
    scale = 1.0 / jnp.sqrt(counts)

    small[0].wait()
    small[1].wait()

    def project(k, ref):
        loads[k][0].wait()
        ref[0:64] = dot(pin[...], hbuf[k])
        loads[k][1].wait()
        ref[64:128] = dot_nt(pout[...], gbuf[k])

    d2d = []
    zsend = []
    up = (c + 1) % 4
    down = (c + 3) % 4

    def zcopy(k, src, to):
        return rc(src, zrecv.at[k], z_s.at[k], z_r.at[k], dp, to * 2 + h)

    def finish(k):
        d2d[k].wait_recv()
        pmine[k] = pmine[k] + precv[k]
        if k == 0:
            zsend.append(zcopy(0, pmine.at[0, 0:64], down))
            zsend.append(zcopy(1, pmine.at[0, 64:128], up))
            launch(zsend[0])
            launch(zsend[1])
        if k == 1:
            zsend.append(zcopy(2, pmine.at[1, 0:64], up))
            launch(zsend[2])
        if k == 2:
            zsend.append(zcopy(3, pmine.at[2, 64:128], down))
            launch(zsend[3])

    for k in range(4):
        project(2 * k, psend.at[k])
        if k == 0:
            pl.semaphore_wait(barrier, DP - 1 + 2 * (MP - 1))
        d2d.append(rc(psend.at[k], precv.at[k], d2d_s.at[k], d2d_r.at[k], dp, partner))
        launch(d2d[k])
        project(2 * k + 1, pmine.at[k])
        if k >= 1:
            finish(k - 1)
    finish(3)

    zsend[0].wait_recv()
    zrel[0] = zrecv[0] + pmine[2, 0:64]
    zsend.append(zcopy(4, zrel.at[0], down))
    launch(zsend[4])
    zsend[1].wait_recv()
    zrel[1] = zrecv[1] + pmine[1, 64:128]
    zsend.append(zcopy(5, zrel.at[1], up))
    launch(zsend[5])
    zsend[2].wait_recv()
    zsend[3].wait_recv()
    zsend[4].wait_recv()
    zsend[5].wait_recv()
    pown[0:64] = pmine[3, 0:64] + zrecv[2] + zrecv[4]
    pown[64:128] = pmine[3, 64:128] + zrecv[3] + zrecv[5]

    px = rc(pown, ppart, px_s, px_r, dp, partner)
    launch(px)

    def weigh(s, toks, blk):
        ih, il = split(toks[0:64])
        base = s * 512
        rb[0:64, base : base + 256] = ih
        rb[64:128, base + 256 : base + 512] = ih
        rb[128:192, base : base + 256] = il
        rb[192:256, base + 256 : base + 512] = il
        ids = seg[:, pl.ds(pl.multiple_of(blk * nblk, nblk), nblk)]
        mask = lax.broadcasted_iota(jnp.int32, (EX, nblk), 0) == ids
        for cq in range(4):
            rows = toks[pl.ds(pl.multiple_of(64 + 16 * cq + 8 * h, 8), 8)]
            for k in range(4):
                tile = (cq * 2 + k % 2) * 2 + k // 2
                for par in range(2):
                    one = jnp.where(mask, rows[2 * k + par : 2 * k + par + 1, :], 0.0)
                    oh, ol = split(one)
                    whi[tile * 16 : tile * 16 + 16, base + par * 256 : base + par * 256 + 256] = oh
                    wlo[tile * 16 : tile * 16 + 16, base + par * 256 : base + par * 256 + 256] = ol

    def grads(s):
        cols = slice(s * 512, s * 512 + 512)
        both = dot_nt(whi[:, cols], rb[:, cols])
        return both[:, 0:128] + both[:, 128:256] + dot_nt(wlo[:, cols], rb[0:128, cols])

    weigh(0, pown, m)
    g0 = grads(0)
    px.wait_recv()
    weigh(1, ppart, partner)
    gbuf2[...] = (g0 + grads(1)).reshape(4, 2, 2, 16, 128)

    bs = []
    for k in (2, 1, 3):
        to = (c + k) % 4
        cp = rc(gbuf2.at[to], brecv.at[k - 1], b_s.at[k - 1], b_r.at[k - 1], dp, to * 2 + h)
        launch(cp)
        bs.append(cp)
    for cp in bs:
        cp.wait_recv()
    fown[...] = (gbuf2[c] + brecv[0] + brecv[1] + brecv[2]) * scale[None, None]

    def c2(k):
        to = (m + k) % MP
        return rc(fown.at[to % 2], fpar.at[m], c2_s.at[k], c2_r.at[k], dp, to)

    def c1(k):
        to = (dp + k) % DP
        return rc(fown.at[to % 2], cc.at[dp], c1_s.at[k], c1_r.at[k], to, m)

    def c3(k):
        to = (dp + k) % DP
        tp = to // 2
        return rc(fpar.at[tp // 2, tp % 2], rr.at[dp], c3_s.at[k], c3_r.at[k], to, m)

    for k in range(1, MP):
        launch(c2(k))
    launch_each(DP, c1)
    cc[dp] = fown[zl]
    fpar[m] = fown[h]
    for k in range(1, MP):
        c2(k).wait_recv()
    launch_each(DP, c3)
    rr[dp] = fpar[p // 2, p % 2]
    ft = rc(fpar, fparp, ft_s, ft_r, dp, partner)
    launch(ft)
    each(DP, lambda k: c3(k).wait_recv())
    c4 = rc(rr, rrp, c4_s, c4_r, dp, partner)
    launch(c4)
    ft.wait_recv()
    for q in range(MP):
        for k2 in range(2):
            col = 4 * q + 2 * k2
            feat_o[:, pl.ds(pl.multiple_of((col + h) * 128, 128), 128)] = fpar[q, k2]
            feat_o[:, pl.ds(pl.multiple_of((col + 1 - h) * 128, 128), 128)] = fparp[q, k2]
    each(DP, lambda k: c1(k).wait_recv())

    cols = [cc[:, k2].reshape(DP * EX, 128) for k2 in range(2)]
    parts = [split(x) for x in cols]
    right = jnp.concatenate([parts[0][0], parts[1][0], parts[0][1], parts[1][1]], axis=1)

    def block(rows, par):
        lh, ll = split(rows[...].reshape(DP * EX, 128).T)
        both = dot(lh, right)
        res = both[:, 0:256] + both[:, 256:512] + dot(ll, right[:, 0:256])
        res = res * (1.0 / (DP * EX))
        for k2 in range(2):
            gb[par, :, k2] = res[:, k2 * 128 : k2 * 128 + 128].reshape(MP, 16, 128)

    block(rr, h)
    c4.wait_recv()
    block(rrp, 1 - h)

    me = zl * MP + m

    def dd(k):
        f = (me + k) % (2 * MP)
        return rc(gb.at[f // MP, f % MP], gg.at[me], dd_s.at[k], dd_r.at[k], 2 * p + f // MP, f % MP)

    for k in range(1, 2 * MP):
        launch(dd(k))
    gg[me] = gb[zl, m]
    for k in range(1, 2 * MP):
        dd(k).wait_recv()
    for s in range(2 * MP):
        for k2 in range(2):
            i2 = 4 * (s % MP) + 2 * k2 + s // MP
            gram_o[:, i2 * 128 : i2 * 128 + 128] = gg[s, k2]
    drain()


def body(hidden, out_grad, proj_in, proj_out, segment_ids):
    hidden = hidden.T
    kin = hidden.shape[0]
    kout = out_grad.shape[1]
    vmem = pl.BlockSpec(memory_space=pltpu.VMEM)
    hbm = pl.BlockSpec(memory_space=pltpu.HBM)
    dma = pltpu.SemaphoreType.DMA
    scratch = [
        pltpu.VMEM(proj_in.shape, BF16),
        pltpu.VMEM(proj_out.shape, BF16),
        pltpu.VMEM(segment_ids.shape, jnp.int32),
        pltpu.VMEM((8, kin, 256), BF16),
        pltpu.VMEM((8, 256, kout), BF16),
        pltpu.VMEM((4, 128, 256), F32),
        pltpu.VMEM((4, 128, 256), F32),
        pltpu.VMEM((4, 128, 256), F32),
        pltpu.VMEM((6, 64, 256), F32),
        pltpu.VMEM((2, 64, 256), F32),
        pltpu.VMEM((128, 256), F32),
        pltpu.VMEM((128, 256), F32),
        pltpu.VMEM((256, 1024), BF16),
        pltpu.VMEM((256, 1024), BF16),
        pltpu.VMEM((256, 1024), BF16),
        pltpu.VMEM((4, 2, 2, 16, 128), F32),
        pltpu.VMEM((3, 2, 2, 16, 128), F32),
        pltpu.VMEM((2, 2, 16, 128), F32),
        pltpu.VMEM((8, 2, 16, 128), F32),
        pltpu.VMEM((8, 2, 16, 128), F32),
        pltpu.VMEM((32, 2, 16, 128), F32),
        pltpu.VMEM((32, 16, 128), F32),
        pltpu.VMEM((32, 16, 128), F32),
        pltpu.VMEM((2, 8, 2, 16, 128), F32),
        pltpu.VMEM((16, 2, 16, 128), F32),
        dma((19,)),
        dma((4,)),
        dma((4,)),
        dma((6,)),
        dma((6,)),
        dma,
        dma,
        dma((3,)),
        dma((3,)),
        dma((32,)),
        dma((32,)),
        dma((8,)),
        dma((8,)),
        dma((32,)),
        dma((32,)),
        dma,
        dma,
        dma,
        dma,
        dma((16,)),
        dma((16,)),
    ]
    return pl.pallas_call(
        kernel,
        out_shape=(
            jax.ShapeDtypeStruct((EX, 4096), F32),
            jax.ShapeDtypeStruct((16, 4096), F32),
        ),
        in_specs=[hbm, hbm, hbm, hbm, hbm],
        out_specs=(vmem, vmem),
        scratch_shapes=scratch,
        compiler_params=pltpu.CompilerParams(
            collective_id=0, has_side_effects=True, vmem_limit_bytes=65800000
        ),
        name="projected_gram",
    )(hidden, out_grad, proj_in, proj_out, segment_ids)


def solution(mesh):
    placed = (P("dp", "mp"), P("dp", "mp"), P(None, "mp"), P(None, "mp"), P("dp", None))
    return jax.shard_map(
        body,
        mesh=mesh,
        in_specs=placed,
        out_specs=(P("dp", None), P(("dp", "mp"), None)),
        check_vma=False,
    )
```

```python
import jax
import jax.numpy as jnp
from jax import lax
from jax.experimental import pallas as pl
from jax.experimental.pallas import tpu as pltpu
from jax.sharding import PartitionSpec as P

MESH = pl.DeviceIdType.MESH
EX = 16
DP = 32
MP = 8
XY = 16
F32 = jnp.float32
BF16 = jnp.bfloat16


def split(x):
    hi = x.astype(BF16)
    return hi, (x - hi.astype(F32)).astype(BF16)


def dot_nt(a, b):
    return lax.dot_general(a, b, (((1,), (1,)), ((), ())), preferred_element_type=F32)


def dot(a, b):
    return lax.dot_general(a, b, (((1,), (0,)), ((), ())), preferred_element_type=F32)


def kernel(
    hid,
    og,
    pin_h,
    pout_h,
    seg_h,
    feat_o,
    gram_o,
    pin,
    pout,
    seg,
    hbuf,
    gbuf,
    psend,
    pmine,
    precv,
    zrecv,
    zrel,
    pown,
    ppart,
    whi,
    wlo,
    rb,
    gbuf2,
    brecv,
    fown,
    fpar,
    fnat,
    fnatp,
    cc,
    ccp,
    rr,
    ath,
    atl,
    gb,
    gg,
    lsem,
    d2d_s,
    d2d_r,
    z_s,
    z_r,
    px_s,
    px_r,
    b_s,
    b_r,
    c1_s,
    c1_r,
    c2_s,
    c2_r,
    c3_s,
    c3_r,
    c4_s,
    c4_r,
    ft_s,
    ft_r,
    dd_s,
    dd_r,
):
    dp = lax.axis_index("dp")
    m = lax.axis_index("mp")
    c = m // 2
    h = m % 2
    p = dp // 2
    zl = dp % 2
    partner = c * 2 + (1 - h)
    nblk = 256

    def rc(src, dst, ss, rs, tdp, tmp):
        return pltpu.make_async_remote_copy(
            src_ref=src,
            dst_ref=dst,
            send_sem=ss,
            recv_sem=rs,
            device_id=(tdp, tmp),
            device_id_type=MESH,
        )

    sent = []

    def drain():
        for wait in sent:
            wait()

    def launch(copy):
        copy.start()
        sent.append(copy.wait_send)

    def launch_each(n, f):
        each(n, lambda k: f(k).start())
        sent.append(lambda: each(n, lambda k: f(k).wait_send()))

    def each(n, f):
        lax.fori_loop(1, n, lambda k, v: (f(k), v)[1], 0)

    owners = [(c + 2) % 4, (c + 1) % 4, (c + 3) % 4, c]
    blocks = []
    for o in owners:
        blocks.append(o * 2 + (1 - h))
        blocks.append(o * 2 + h)
    small = []
    for k, (src, dst) in enumerate(((pin_h, pin), (pout_h, pout), (seg_h, seg))):
        small.append(pltpu.make_async_copy(src, dst, lsem.at[16 + k]))
        small[k].start()
    loads = []
    for k, blk in enumerate(blocks):
        rows = pl.ds(pl.multiple_of(blk * nblk, nblk), nblk)
        a = pltpu.make_async_copy(hid.at[:, rows], hbuf.at[k], lsem.at[2 * k])
        b = pltpu.make_async_copy(og.at[rows], gbuf.at[k], lsem.at[2 * k + 1])
        a.start()
        b.start()
        loads.append((a, b))

    barrier = pltpu.get_barrier_semaphore()

    def greet_dp(k, carry):
        pl.semaphore_signal(barrier, inc=1, device_id=((dp + k) % DP, m), device_id_type=MESH)
        return carry

    lax.fori_loop(1, DP, greet_dp, 0)

    def greet_own(k, carry):
        pl.semaphore_signal(barrier, inc=1, device_id=(dp, (m + k) % MP), device_id_type=MESH)
        return carry

    lax.fori_loop(1, MP, greet_own, 0)

    def greet_plane(k, carry):
        pl.semaphore_signal(
            barrier, inc=1, device_id=((p + k) % XY * 2 + zl, partner), device_id_type=MESH
        )
        return carry

    lax.fori_loop(1, XY, greet_plane, 0)

    rb[...] = jnp.zeros(rb.shape, BF16)

    small[2].wait()
    segv = seg[...]
    erow = lax.broadcasted_iota(jnp.int32, (EX, segv.shape[1]), 0)
    counts = jnp.sum(jnp.where(erow == segv, 1.0, 0.0).astype(F32), axis=1, keepdims=True)
    scale = 1.0 / jnp.sqrt(counts)

    small[0].wait()
    small[1].wait()

    def project(k, ref):
        loads[k][0].wait()
        ref[0:64] = dot(pin[...], hbuf[k])
        loads[k][1].wait()
        ref[64:128] = dot_nt(pout[...], gbuf[k])

    d2d = []
    zsend = []
    up = (c + 1) % 4
    down = (c + 3) % 4

    def zcopy(k, src, to):
        return rc(src, zrecv.at[k], z_s.at[k], z_r.at[k], dp, to * 2 + h)

    def finish(k):
        d2d[k].wait_recv()
        pmine[k] = pmine[k] + precv[k]
        if k == 0:
            zsend.append(zcopy(0, pmine.at[0, 0:64], down))
            zsend.append(zcopy(1, pmine.at[0, 64:128], up))
            launch(zsend[0])
            launch(zsend[1])
        if k == 1:
            zsend.append(zcopy(2, pmine.at[1, 0:64], up))
            launch(zsend[2])
        if k == 2:
            zsend.append(zcopy(3, pmine.at[2, 64:128], down))
            launch(zsend[3])

    for k in range(4):
        project(2 * k, psend.at[k])
        if k == 0:
            pl.semaphore_wait(barrier, DP - 1 + MP - 1 + XY - 1)
        d2d.append(rc(psend.at[k], precv.at[k], d2d_s.at[k], d2d_r.at[k], dp, partner))
        launch(d2d[k])
        project(2 * k + 1, pmine.at[k])
        if k >= 1:
            finish(k - 1)
    finish(3)

    zsend[0].wait_recv()
    zrel[0] = zrecv[0] + pmine[2, 0:64]
    zsend.append(zcopy(4, zrel.at[0], down))
    launch(zsend[4])
    zsend[1].wait_recv()
    zrel[1] = zrecv[1] + pmine[1, 64:128]
    zsend.append(zcopy(5, zrel.at[1], up))
    launch(zsend[5])
    zsend[2].wait_recv()
    zsend[3].wait_recv()
    zsend[4].wait_recv()
    zsend[5].wait_recv()
    pown[0:64] = pmine[3, 0:64] + zrecv[2] + zrecv[4]
    pown[64:128] = pmine[3, 64:128] + zrecv[3] + zrecv[5]

    px = rc(pown, ppart, px_s, px_r, dp, partner)
    launch(px)

    def weigh(s, toks, blk):
        ih, il = split(toks[0:64])
        base = s * 512
        rb[0:64, base : base + 256] = ih
        rb[64:128, base + 256 : base + 512] = ih
        rb[128:192, base : base + 256] = il
        rb[192:256, base + 256 : base + 512] = il
        ids = seg[:, pl.ds(pl.multiple_of(blk * nblk, nblk), nblk)]
        mask = lax.broadcasted_iota(jnp.int32, (EX, nblk), 0) == ids
        rows = toks[pl.ds(pl.multiple_of(64 + 32 * h, 32), 32)]
        for t in range(16):
            for par in range(2):
                one = jnp.where(mask, rows[2 * t + par : 2 * t + par + 1, :], 0.0)
                oh, ol = split(one)
                whi[t * 16 : t * 16 + 16, base + par * 256 : base + par * 256 + 256] = oh
                wlo[t * 16 : t * 16 + 16, base + par * 256 : base + par * 256 + 256] = ol

    def grads(s):
        cols = slice(s * 512, s * 512 + 512)
        both = dot_nt(whi[:, cols], rb[:, cols])
        return both[:, 0:128] + both[:, 128:256] + dot_nt(wlo[:, cols], rb[0:128, cols])

    weigh(0, pown, m)
    g0 = grads(0)
    px.wait_recv()
    weigh(1, ppart, partner)
    nat = (g0 + grads(1)).reshape(16, EX, 128)
    group = lax.broadcasted_iota(jnp.int32, (EX, 128), 1) // 32

    def regroup(tiles, here):
        out = None
        for g in range(4):
            moved = tiles[g] if g == here else pltpu.roll(tiles[g], 32 * ((g - here) % 4), 1)
            out = moved if out is None else jnp.where(group == g, moved, out)
        return out

    for cq in range(4):
        for z in range(2):
            for k in range(2):
                gbuf2[cq, z, k] = regroup([nat[8 * k + 2 * g + z] for g in range(4)], cq)

    bs = []
    for k in (2, 1, 3):
        to = (c + k) % 4
        cp = rc(gbuf2.at[to], brecv.at[k - 1], b_s.at[k - 1], b_r.at[k - 1], dp, to * 2 + h)
        launch(cp)
        bs.append(cp)
    for cp in bs:
        cp.wait_recv()
    fown[...] = (gbuf2[c] + brecv[0] + brecv[1] + brecv[2]) * scale[None, None]

    other = 2 * p + 1 - zl

    def c2(k):
        to = (m + k) % MP
        return rc(fown.at[to % 2], fpar.at[m], c2_s.at[k], c2_r.at[k], dp, to)

    def c1(k):
        to = (p + k) % XY * 2 + zl
        return rc(fown.at[zl], cc.at[zl, p], c1_s.at[k], c1_r.at[k], to, m)

    def c1b(k):
        to = (p + k) % XY * 2 + zl
        mid = cc.at[1 - zl, p]
        return rc(mid, mid, c1_s.at[16 + k], c1_r.at[16 + k], to, m)

    def c3(k):
        to = (dp + k) % DP
        return rc(fnat.at[to // 2], rr.at[zl, p], c3_s.at[k], c3_r.at[k], to, m)

    for k in range(1, MP):
        launch(c2(k))
    x1 = rc(fown.at[1 - zl], cc.at[zl, p], c1_s.at[0], c1_r.at[0], other, m)
    launch(x1)
    launch_each(XY, c1)
    cc[zl, p] = fown[zl]
    fpar[m] = fown[h]
    x1.wait_recv()
    launch_each(XY, c1b)
    for k in range(1, MP):
        c2(k).wait_recv()
    for q in range(4):
        for g in range(4):
            fnat[4 * q + g] = regroup([fpar[2 * cq + q // 2, q % 2] for cq in range(4)], g)
    launch_each(DP, c3)
    rr[zl, p] = fnat[p]
    ft = rc(fnat, fnatp, ft_s, ft_r, dp, partner)
    launch(ft)

    def swap(z):
        return rc(cc.at[z], ccp.at[z], c4_s.at[z], c4_r.at[z], dp, partner)

    each(XY, lambda k: c1(k).wait_recv())
    launch(swap(zl))
    each(XY, lambda k: c1b(k).wait_recv())
    launch(swap(1 - zl))
    ft.wait_recv()
    for q in range(XY):
        feat_o[:, pl.ds(pl.multiple_of((2 * q + h) * 128, 128), 128)] = fnat[q]
        feat_o[:, pl.ds(pl.multiple_of((2 * q + 1 - h) * 128, 128), 128)] = fnatp[q]

    def turned(ref, side):
        for k in range(2):
            for z in range(2):
                hi, lo = split(ref[z, :, k].reshape(XY * EX, 128).T)
                ath[side, k * 128 : k * 128 + 128, z * 256 : z * 256 + 256] = hi
                atl[side, k * 128 : k * 128 + 128, z * 256 : z * 256 + 256] = lo

    turned(cc, 0)
    swap(zl).wait_recv()
    swap(1 - zl).wait_recv()
    turned(ccp, 1)
    each(DP, lambda k: c3(k).wait_recv())
    rh, rl = split(rr[...].reshape(DP * EX, 128))
    right = jnp.concatenate([rh, rl], axis=1)
    for side in range(2):
        both = dot(ath[side], right)
        res = both[:, 0:128] + both[:, 128:256] + dot(atl[side], rh)
        res = (res * (1.0 / (DP * EX))).reshape(2, 4, 2, 16, 128)
        first = h if side == 0 else 1 - h
        gb[pl.ds(2 * first, 2)] = res

    me = 2 * p + h

    def dd(k):
        f = (me + k) % DP
        return rc(
            gb.at[f // 8, f // 2 % 4, f % 2],
            gg.at[me],
            dd_s.at[k],
            dd_r.at[k],
            f // 2 * 2 + zl,
            2 * c + f % 2,
        )

    launch_each(DP, dd)
    gg[me] = gb[p // 4, p % 4, h]
    each(DP, lambda k: dd(k).wait_recv())
    for i in range(DP):
        gram_o[:, i * 128 : i * 128 + 128] = gg[i]

    drain()


def body(hidden, out_grad, proj_in, proj_out, segment_ids):
    hidden = hidden.T
    kin = hidden.shape[0]
    kout = out_grad.shape[1]
    vmem = pl.BlockSpec(memory_space=pltpu.VMEM)
    hbm = pl.BlockSpec(memory_space=pltpu.HBM)
    dma = pltpu.SemaphoreType.DMA
    scratch = [
        pltpu.VMEM(proj_in.shape, BF16),
        pltpu.VMEM(proj_out.shape, BF16),
        pltpu.VMEM(segment_ids.shape, jnp.int32),
        pltpu.VMEM((8, kin, 256), BF16),
        pltpu.VMEM((8, 256, kout), BF16),
        pltpu.VMEM((4, 128, 256), F32),
        pltpu.VMEM((4, 128, 256), F32),
        pltpu.VMEM((4, 128, 256), F32),
        pltpu.VMEM((6, 64, 256), F32),
        pltpu.VMEM((2, 64, 256), F32),
        pltpu.VMEM((128, 256), F32),
        pltpu.VMEM((128, 256), F32),
        pltpu.VMEM((256, 1024), BF16),
        pltpu.VMEM((256, 1024), BF16),
        pltpu.VMEM((256, 1024), BF16),
        pltpu.VMEM((4, 2, 2, 16, 128), F32),
        pltpu.VMEM((3, 2, 2, 16, 128), F32),
        pltpu.VMEM((2, 2, 16, 128), F32),
        pltpu.VMEM((8, 2, 16, 128), F32),
        pltpu.VMEM((16, 16, 128), F32),
        pltpu.VMEM((16, 16, 128), F32),
        pltpu.VMEM((2, 16, 2, 16, 128), F32),
        pltpu.VMEM((2, 16, 2, 16, 128), F32),
        pltpu.VMEM((2, 16, 16, 128), F32),
        pltpu.VMEM((2, 256, 512), BF16),
        pltpu.VMEM((2, 256, 512), BF16),
        pltpu.VMEM((4, 4, 2, 16, 128), F32),
        pltpu.VMEM((32, 16, 128), F32),
        dma((19,)),
        dma((4,)),
        dma((4,)),
        dma((6,)),
        dma((6,)),
        dma,
        dma,
        dma((3,)),
        dma((3,)),
        dma((32,)),
        dma((32,)),
        dma((8,)),
        dma((8,)),
        dma((32,)),
        dma((32,)),
        dma((2,)),
        dma((2,)),
        dma,
        dma,
        dma((32,)),
        dma((32,)),
    ]
    return pl.pallas_call(
        kernel,
        out_shape=(
            jax.ShapeDtypeStruct((EX, 4096), F32),
            jax.ShapeDtypeStruct((16, 4096), F32),
        ),
        in_specs=[hbm, hbm, hbm, hbm, hbm],
        out_specs=(vmem, vmem),
        scratch_shapes=scratch,
        compiler_params=pltpu.CompilerParams(
            collective_id=0, has_side_effects=True, vmem_limit_bytes=65800000
        ),
        name="projected_gram",
    )(hidden, out_grad, proj_in, proj_out, segment_ids)


def solution(mesh):
    placed = (P("dp", "mp"), P("dp", "mp"), P(None, "mp"), P(None, "mp"), P("dp", None))
    return jax.shard_map(
        body,
        mesh=mesh,
        in_specs=placed,
        out_specs=(P("dp", None), P(("dp", "mp"), None)),
        check_vma=False,
    )
```

```python
import jax
import jax.numpy as jnp
from jax import lax
from jax.experimental import pallas as pl
from jax.experimental.pallas import tpu as pltpu
from jax.sharding import PartitionSpec as P

MESH = pl.DeviceIdType.MESH
EX = 16
DP = 32
MP = 8
XY = 16
F32 = jnp.float32
BF16 = jnp.bfloat16


def split(x):
    hi = x.astype(BF16)
    return hi, (x - hi.astype(F32)).astype(BF16)


def dot_nt(a, b):
    return lax.dot_general(a, b, (((1,), (1,)), ((), ())), preferred_element_type=F32)


def dot(a, b):
    return lax.dot_general(a, b, (((1,), (0,)), ((), ())), preferred_element_type=F32)


def kernel(
    hid,
    og,
    pin_h,
    pout_h,
    seg_h,
    feat_o,
    gram_o,
    pin,
    pout,
    seg,
    hbuf,
    gbuf,
    psend,
    pmine,
    precv,
    zrecv,
    zrel,
    pown,
    ppart,
    whi,
    wlo,
    rb,
    gbuf2,
    brecv,
    fown,
    fpar,
    fnat,
    fnatp,
    cc,
    ccp,
    rr,
    ath,
    atl,
    gb,
    gg,
    lsem,
    d2d_s,
    d2d_r,
    z_s,
    z_r,
    px_s,
    px_r,
    b_s,
    b_r,
    c1_s,
    c1_r,
    c2_s,
    c2_r,
    c3_s,
    c3_r,
    c4_s,
    c4_r,
    ft_s,
    ft_r,
    dd_s,
    dd_r,
):
    dp = lax.axis_index("dp")
    m = lax.axis_index("mp")
    c = m // 2
    h = m % 2
    p = dp // 2
    zl = dp % 2
    partner = c * 2 + (1 - h)
    nblk = 256

    def rc(src, dst, ss, rs, tdp, tmp):
        return pltpu.make_async_remote_copy(
            src_ref=src,
            dst_ref=dst,
            send_sem=ss,
            recv_sem=rs,
            device_id=(tdp, tmp),
            device_id_type=MESH,
        )

    sent = []

    def drain():
        for wait in sent:
            wait()

    def launch(copy):
        copy.start()
        sent.append(copy.wait_send)

    def launch_each(n, f):
        each(n, lambda k: f(k).start())
        sent.append(lambda: each(n, lambda k: f(k).wait_send()))

    def each(n, f):
        lax.fori_loop(1, n, lambda k, v: (f(k), v)[1], 0)

    owners = [(c + 2) % 4, (c + 1) % 4, (c + 3) % 4, c]
    blocks = []
    for o in owners:
        blocks.append(o * 2 + (1 - h))
        blocks.append(o * 2 + h)
    small = []
    for k, (src, dst) in enumerate(((pin_h, pin), (pout_h, pout), (seg_h, seg))):
        small.append(pltpu.make_async_copy(src, dst, lsem.at[16 + k]))
        small[k].start()
    loads = []
    for k, blk in enumerate(blocks):
        rows = pl.ds(pl.multiple_of(blk * nblk, nblk), nblk)
        a = pltpu.make_async_copy(hid.at[:, rows], hbuf.at[k], lsem.at[2 * k])
        b = pltpu.make_async_copy(og.at[rows], gbuf.at[k], lsem.at[2 * k + 1])
        a.start()
        b.start()
        loads.append((a, b))

    barrier = pltpu.get_barrier_semaphore()

    def greet_dp(k, carry):
        pl.semaphore_signal(barrier, inc=1, device_id=((dp + k) % DP, m), device_id_type=MESH)
        return carry

    lax.fori_loop(1, DP, greet_dp, 0)

    def greet_own(k, carry):
        pl.semaphore_signal(barrier, inc=1, device_id=(dp, (m + k) % MP), device_id_type=MESH)
        return carry

    lax.fori_loop(1, MP, greet_own, 0)

    def greet_plane(k, carry):
        pl.semaphore_signal(
            barrier, inc=1, device_id=((p + k) % XY * 2 + zl, partner), device_id_type=MESH
        )
        return carry

    lax.fori_loop(1, XY, greet_plane, 0)

    rb[...] = jnp.zeros(rb.shape, BF16)

    small[2].wait()
    segv = seg[...]
    erow = lax.broadcasted_iota(jnp.int32, (EX, segv.shape[1]), 0)
    counts = jnp.sum(jnp.where(erow == segv, 1.0, 0.0).astype(F32), axis=1, keepdims=True)
    scale = 1.0 / jnp.sqrt(counts)

    small[0].wait()
    small[1].wait()

    def project(k, ref):
        loads[k][0].wait()
        ref[0:64] = dot(pin[...], hbuf[k])
        loads[k][1].wait()
        ref[64:128] = dot_nt(pout[...], gbuf[k])

    d2d = []
    zsend = []
    up = (c + 1) % 4
    down = (c + 3) % 4

    def zcopy(k, src, to):
        return rc(src, zrecv.at[k], z_s.at[k], z_r.at[k], dp, to * 2 + h)

    def finish(k):
        d2d[k].wait_recv()
        pmine[k] = pmine[k] + precv[k]
        if k == 0:
            zsend.append(zcopy(0, pmine.at[0, 0:64], down))
            zsend.append(zcopy(1, pmine.at[0, 64:128], up))
            launch(zsend[0])
            launch(zsend[1])
        if k == 1:
            zsend.append(zcopy(2, pmine.at[1, 0:64], up))
            launch(zsend[2])
        if k == 2:
            zsend.append(zcopy(3, pmine.at[2, 64:128], down))
            launch(zsend[3])

    for k in range(4):
        project(2 * k, psend.at[k])
        if k == 0:
            pl.semaphore_wait(barrier, DP - 1 + MP - 1 + XY - 1)
        d2d.append(rc(psend.at[k], precv.at[k], d2d_s.at[k], d2d_r.at[k], dp, partner))
        launch(d2d[k])
        project(2 * k + 1, pmine.at[k])
        if k >= 1:
            finish(k - 1)
    finish(3)

    zsend[0].wait_recv()
    zrel[0] = zrecv[0] + pmine[2, 0:64]
    zsend.append(zcopy(4, zrel.at[0], down))
    launch(zsend[4])
    zsend[1].wait_recv()
    zrel[1] = zrecv[1] + pmine[1, 64:128]
    zsend.append(zcopy(5, zrel.at[1], up))
    launch(zsend[5])
    zsend[2].wait_recv()
    zsend[3].wait_recv()
    zsend[4].wait_recv()
    zsend[5].wait_recv()
    pown[0:64] = pmine[3, 0:64] + zrecv[2] + zrecv[4]
    pown[64:128] = pmine[3, 64:128] + zrecv[3] + zrecv[5]

    px = rc(pown, ppart, px_s, px_r, dp, partner)
    launch(px)

    def weigh(s, toks, blk):
        ih, il = split(toks[0:64])
        base = s * 512
        rb[0:64, base : base + 256] = ih
        rb[64:128, base + 256 : base + 512] = ih
        rb[128:192, base : base + 256] = il
        rb[192:256, base + 256 : base + 512] = il
        ids = seg[:, pl.ds(pl.multiple_of(blk * nblk, nblk), nblk)]
        mask = lax.broadcasted_iota(jnp.int32, (EX, nblk), 0) == ids
        rows = toks[pl.ds(pl.multiple_of(64 + 32 * h, 32), 32)]
        for t in range(16):
            for par in range(2):
                one = jnp.where(mask, rows[2 * t + par : 2 * t + par + 1, :], 0.0)
                oh, ol = split(one)
                whi[t * 16 : t * 16 + 16, base + par * 256 : base + par * 256 + 256] = oh
                wlo[t * 16 : t * 16 + 16, base + par * 256 : base + par * 256 + 256] = ol

    def grads(s):
        cols = slice(s * 512, s * 512 + 512)
        both = dot_nt(whi[:, cols], rb[:, cols])
        return both[:, 0:128] + both[:, 128:256] + dot_nt(wlo[:, cols], rb[0:128, cols])

    weigh(0, pown, m)
    g0 = grads(0)
    px.wait_recv()
    weigh(1, ppart, partner)
    nat = (g0 + grads(1)).reshape(16, EX, 128)
    group = lax.broadcasted_iota(jnp.int32, (EX, 128), 1) // 32

    def regroup(tiles, here):
        out = None
        for g in range(4):
            moved = tiles[g] if g == here else pltpu.roll(tiles[g], 32 * ((g - here) % 4), 1)
            out = moved if out is None else jnp.where(group == g, moved, out)
        return out

    for cq in range(4):
        for z in range(2):
            for k in range(2):
                gbuf2[cq, z, k] = regroup([nat[8 * k + 2 * g + z] for g in range(4)], cq)

    bs = []
    for k in (2, 1, 3):
        to = (c + k) % 4
        cp = rc(gbuf2.at[to], brecv.at[k - 1], b_s.at[k - 1], b_r.at[k - 1], dp, to * 2 + h)
        launch(cp)
        bs.append(cp)
    for cp in bs:
        cp.wait_recv()
    fown[...] = (gbuf2[c] + brecv[0] + brecv[1] + brecv[2]) * scale[None, None]

    far = (2, 1, 3, 0)
    yy = p // 4
    xx = p % 4
    u = yy * (1 - h) + xx * h
    v = xx * (1 - h) + yy * h

    def spot(first, second):
        return (first * (4 - 3 * h) + second * (1 + 3 * h)) * 2 + zl

    def c2(k):
        to = (m + k) % MP
        return rc(fown.at[to % 2], fpar.at[m], c2_s.at[k], c2_r.at[k], dp, to)

    def near(z, k):
        src = fown.at[zl] if z == 0 else cc.at[1 - zl, u, v]
        dst = cc.at[(zl + z) % 2, u, v]
        n = 1 + z * 6 + k
        return rc(src, dst, c1_s.at[n], c1_r.at[n], spot(u, (v + k) % 4), m)

    def wide(z, k):
        row = cc.at[(zl + z) % 2, u]
        n = 4 + z * 6 + k
        return rc(row, row, c1_s.at[n], c1_r.at[n], spot((u + k) % 4, v), m)

    def c3(k):
        tp = (yy + k // 8) % 4 * 4 + (xx + k // 2 % 4) % 4
        to = tp * 2 + (zl + k % 2) % 2
        return rc(fnat.at[tp], rr.at[zl, p], c3_s.at[k], c3_r.at[k], to, m)

    def dd(k):
        ty = (yy + k // 8) % 4
        tx = (xx + k // 2 % 4) % 4
        th = (h + k % 2) % 2
        return rc(
            gb.at[ty, tx, th],
            gg.at[2 * p + h],
            dd_s.at[k],
            dd_r.at[k],
            (ty * 4 + tx) * 2 + zl,
            2 * c + th,
        )

    for k in (4, 5, 3, 2, 6, 7, 1):
        launch(c2(k))
    x1 = rc(fown.at[1 - zl], cc.at[zl, u, v], c1_s.at[0], c1_r.at[0], 2 * p + 1 - zl, m)
    launch(x1)
    for k in far[:3]:
        launch(near(0, k))
    cc[zl, u, v] = fown[zl]
    fpar[m] = fown[h]
    x1.wait_recv()
    for k in far[:3]:
        launch(near(1, k))
    for z in range(2):
        for k in far[:3]:
            near(z, k).wait_recv()
        for k in far[:3]:
            launch(wide(z, k))
    for k in range(1, MP):
        c2(k).wait_recv()
    for q in range(4):
        for g in range(4):
            fnat[4 * q + g] = regroup([fpar[2 * cq + q // 2, q % 2] for cq in range(4)], g)
    for dz in (1, 0):
        for dy in far:
            for dx in far:
                if dy + dx + dz:
                    c3(dy * 8 + dx * 2 + dz).start()
    sent.append(lambda: each(DP, lambda k: c3(k).wait_send()))
    rr[zl, p] = fnat[p]
    ft = rc(fnat, fnatp, ft_s, ft_r, dp, partner)
    launch(ft)

    def swap(z):
        return rc(cc.at[z], ccp.at[z], c4_s.at[z], c4_r.at[z], dp, partner)

    for z in range(2):
        for k in far[:3]:
            wide(z, k).wait_recv()
        launch(swap((zl + z) % 2))
    ft.wait_recv()
    for q in range(XY):
        feat_o[:, pl.ds(pl.multiple_of((2 * q + h) * 128, 128), 128)] = fnat[q]
        feat_o[:, pl.ds(pl.multiple_of((2 * q + 1 - h) * 128, 128), 128)] = fnatp[q]

    def turned(ref, core):
        for k in range(2):
            for z in range(2):
                tiles = []
                for y in range(4):
                    for x in range(4):
                        first = y * (1 - core) + x * core
                        second = x * (1 - core) + y * core
                        tiles.append(ref[z, first, second, k])
                hi, lo = split(jnp.concatenate(tiles, axis=0).T)
                ath[2 * core + k, :, z * 256 : z * 256 + 256] = hi
                atl[2 * core + k, :, z * 256 : z * 256 + 256] = lo

    turned(cc, h)
    swap(zl).wait_recv()
    swap(1 - zl).wait_recv()
    turned(ccp, 1 - h)
    each(DP, lambda k: c3(k).wait_recv())
    rh, rl = split(rr[...].reshape(DP * EX, 128))
    right = jnp.concatenate([rh, rl], axis=1)
    for dy in far:
        q = (yy + dy) % 4
        both = dot(ath[q], right)
        res = both[:, 0:128] + both[:, 128:256] + dot(atl[q], rh)
        gb[q] = (res * (1.0 / (DP * EX))).reshape(4, 2, 16, 128)
        for dx in far:
            for dh in (1, 0):
                if dy + dx + dh:
                    dd(dy * 8 + dx * 2 + dh).start()
    sent.append(lambda: each(DP, lambda k: dd(k).wait_send()))
    gg[2 * p + h] = gb[yy, xx, h]
    each(DP, lambda k: dd(k).wait_recv())
    for i in range(DP):
        gram_o[:, i * 128 : i * 128 + 128] = gg[i]

    drain()


def body(hidden, out_grad, proj_in, proj_out, segment_ids):
    hidden = hidden.T
    kin = hidden.shape[0]
    kout = out_grad.shape[1]
    vmem = pl.BlockSpec(memory_space=pltpu.VMEM)
    hbm = pl.BlockSpec(memory_space=pltpu.HBM)
    dma = pltpu.SemaphoreType.DMA
    scratch = [
        pltpu.VMEM(proj_in.shape, BF16),
        pltpu.VMEM(proj_out.shape, BF16),
        pltpu.VMEM(segment_ids.shape, jnp.int32),
        pltpu.VMEM((8, kin, 256), BF16),
        pltpu.VMEM((8, 256, kout), BF16),
        pltpu.VMEM((4, 128, 256), F32),
        pltpu.VMEM((4, 128, 256), F32),
        pltpu.VMEM((4, 128, 256), F32),
        pltpu.VMEM((6, 64, 256), F32),
        pltpu.VMEM((2, 64, 256), F32),
        pltpu.VMEM((128, 256), F32),
        pltpu.VMEM((128, 256), F32),
        pltpu.VMEM((256, 1024), BF16),
        pltpu.VMEM((256, 1024), BF16),
        pltpu.VMEM((256, 1024), BF16),
        pltpu.VMEM((4, 2, 2, 16, 128), F32),
        pltpu.VMEM((3, 2, 2, 16, 128), F32),
        pltpu.VMEM((2, 2, 16, 128), F32),
        pltpu.VMEM((8, 2, 16, 128), F32),
        pltpu.VMEM((16, 16, 128), F32),
        pltpu.VMEM((16, 16, 128), F32),
        pltpu.VMEM((2, 4, 4, 2, 16, 128), F32),
        pltpu.VMEM((2, 4, 4, 2, 16, 128), F32),
        pltpu.VMEM((2, 16, 16, 128), F32),
        pltpu.VMEM((4, 128, 512), BF16),
        pltpu.VMEM((4, 128, 512), BF16),
        pltpu.VMEM((4, 4, 2, 16, 128), F32),
        pltpu.VMEM((32, 16, 128), F32),
        dma((19,)),
        dma((4,)),
        dma((4,)),
        dma((6,)),
        dma((6,)),
        dma,
        dma,
        dma((3,)),
        dma((3,)),
        dma((32,)),
        dma((32,)),
        dma((8,)),
        dma((8,)),
        dma((32,)),
        dma((32,)),
        dma((2,)),
        dma((2,)),
        dma,
        dma,
        dma((32,)),
        dma((32,)),
    ]
    return pl.pallas_call(
        kernel,
        out_shape=(
            pltpu.VMEM((EX, 4096), F32),
            pltpu.VMEM((16, 4096), F32),
        ),
        in_specs=[hbm, hbm, hbm, hbm, hbm],
        out_specs=(vmem, vmem),
        scratch_shapes=scratch,
        compiler_params=pltpu.CompilerParams(
            collective_id=0, has_side_effects=True, vmem_limit_bytes=65800000
        ),
        name="projected_gram",
    )(hidden, out_grad, proj_in, proj_out, segment_ids)


def solution(mesh):
    placed = (P("dp", "mp"), P("dp", "mp"), P(None, "mp"), P(None, "mp"), P("dp", None))
    return jax.shard_map(
        body,
        mesh=mesh,
        in_specs=placed,
        out_specs=(P("dp", None), P(("dp", "mp"), None)),
        check_vma=False,
    )
```

```python
import jax
import jax.numpy as jnp
from jax import lax
from jax.experimental import pallas as pl
from jax.experimental.pallas import tpu as pltpu
from jax.sharding import PartitionSpec as P

MESH = pl.DeviceIdType.MESH
EX = 16
DP = 32
MP = 8
XY = 16
F32 = jnp.float32
BF16 = jnp.bfloat16


def split(x):
    hi = x.astype(BF16)
    return hi, (x - hi.astype(F32)).astype(BF16)


def dot_nt(a, b):
    return lax.dot_general(a, b, (((1,), (1,)), ((), ())), preferred_element_type=F32)


def dot(a, b):
    return lax.dot_general(a, b, (((1,), (0,)), ((), ())), preferred_element_type=F32)


def kernel(
    hid,
    og,
    pin_h,
    pout_h,
    seg_h,
    feat_o,
    gram_o,
    pin,
    pout,
    seg,
    hbuf,
    gbuf,
    psend,
    pmine,
    precv,
    zrecv,
    zrel,
    pown,
    ppart,
    whi,
    wlo,
    rb,
    gbuf2,
    brecv,
    fown,
    fpar,
    fnat,
    fnatp,
    cc,
    ccp,
    rr,
    ath,
    atl,
    gb,
    gg,
    lsem,
    d2d_s,
    d2d_r,
    z_s,
    z_r,
    px_s,
    px_r,
    b_s,
    b_r,
    c1_s,
    c1_r,
    c2_s,
    c2_r,
    c3_s,
    c3_r,
    c4_s,
    c4_r,
    ft_s,
    ft_r,
    dd_s,
    dd_r,
):
    dp = lax.axis_index("dp")
    m = lax.axis_index("mp")
    c = m // 2
    h = m % 2
    p = dp // 2
    zl = dp % 2
    partner = c * 2 + (1 - h)
    nblk = 256

    def rc(src, dst, ss, rs, tdp, tmp):
        return pltpu.make_async_remote_copy(
            src_ref=src,
            dst_ref=dst,
            send_sem=ss,
            recv_sem=rs,
            device_id=(tdp, tmp),
            device_id_type=MESH,
        )

    sent = []

    def drain():
        for wait in sent:
            wait()

    def launch(copy):
        copy.start()
        sent.append(copy.wait_send)

    def launch_each(n, f):
        each(n, lambda k: f(k).start())
        sent.append(lambda: each(n, lambda k: f(k).wait_send()))

    def each(n, f):
        lax.fori_loop(1, n, lambda k, v: (f(k), v)[1], 0)

    owners = [(c + 2) % 4, (c + 1) % 4, (c + 3) % 4, c]
    blocks = []
    for o in owners:
        blocks.append(o * 2 + (1 - h))
        blocks.append(o * 2 + h)
    small = []
    for k, (src, dst) in enumerate(((pin_h, pin), (pout_h, pout), (seg_h, seg))):
        small.append(pltpu.make_async_copy(src, dst, lsem.at[16 + k]))
        small[k].start()
    loads = []
    for k, blk in enumerate(blocks):
        rows = pl.ds(pl.multiple_of(blk * nblk, nblk), nblk)
        a = pltpu.make_async_copy(hid.at[:, rows], hbuf.at[k], lsem.at[2 * k])
        b = pltpu.make_async_copy(og.at[rows], gbuf.at[k], lsem.at[2 * k + 1])
        a.start()
        b.start()
        loads.append((a, b))

    barrier = pltpu.get_barrier_semaphore()

    def greet_dp(k, carry):
        pl.semaphore_signal(barrier, inc=1, device_id=((dp + k) % DP, m), device_id_type=MESH)
        return carry

    lax.fori_loop(1, DP, greet_dp, 0)

    def greet_own(k, carry):
        pl.semaphore_signal(barrier, inc=1, device_id=(dp, (m + k) % MP), device_id_type=MESH)
        return carry

    lax.fori_loop(1, MP, greet_own, 0)

    def greet_plane(k, carry):
        pl.semaphore_signal(
            barrier, inc=1, device_id=((p + k) % XY * 2 + zl, partner), device_id_type=MESH
        )
        return carry

    lax.fori_loop(1, XY, greet_plane, 0)

    rb[...] = jnp.zeros(rb.shape, BF16)

    small[2].wait()
    segv = seg[...]
    erow = lax.broadcasted_iota(jnp.int32, (EX, segv.shape[1]), 0)
    counts = jnp.sum(jnp.where(erow == segv, 1.0, 0.0).astype(F32), axis=1, keepdims=True)
    scale = 1.0 / jnp.sqrt(counts)

    small[0].wait()
    small[1].wait()

    def project(k, ref):
        loads[k][0].wait()
        ref[0:64] = dot(pin[...], hbuf[k])
        loads[k][1].wait()
        ref[64:128] = dot_nt(pout[...], gbuf[k])

    d2d = []
    zsend = []
    up = (c + 1) % 4
    down = (c + 3) % 4

    def zcopy(k, src, to):
        return rc(src, zrecv.at[k], z_s.at[k], z_r.at[k], dp, to * 2 + h)

    def finish(k):
        d2d[k].wait_recv()
        pmine[k] = pmine[k] + precv[k]
        if k == 0:
            zsend.append(zcopy(0, pmine.at[0, 0:64], down))
            zsend.append(zcopy(1, pmine.at[0, 64:128], up))
            launch(zsend[0])
            launch(zsend[1])
        if k == 1:
            zsend.append(zcopy(2, pmine.at[1, 0:64], up))
            launch(zsend[2])
        if k == 2:
            zsend.append(zcopy(3, pmine.at[2, 64:128], down))
            launch(zsend[3])

    for k in range(4):
        project(2 * k, psend.at[k])
        if k == 0:
            pl.semaphore_wait(barrier, DP - 1 + MP - 1 + XY - 1)
        d2d.append(rc(psend.at[k], precv.at[k], d2d_s.at[k], d2d_r.at[k], dp, partner))
        launch(d2d[k])
        project(2 * k + 1, pmine.at[k])
        if k >= 1:
            finish(k - 1)
    finish(3)

    zsend[0].wait_recv()
    zrel[0] = zrecv[0] + pmine[2, 0:64]
    zsend.append(zcopy(4, zrel.at[0], down))
    launch(zsend[4])
    zsend[1].wait_recv()
    zrel[1] = zrecv[1] + pmine[1, 64:128]
    zsend.append(zcopy(5, zrel.at[1], up))
    launch(zsend[5])
    zsend[2].wait_recv()
    zsend[3].wait_recv()
    zsend[4].wait_recv()
    zsend[5].wait_recv()
    pown[0:64] = pmine[3, 0:64] + zrecv[2] + zrecv[4]
    pown[64:128] = pmine[3, 64:128] + zrecv[3] + zrecv[5]

    px = rc(pown, ppart, px_s, px_r, dp, partner)
    launch(px)

    def weigh(s, toks, blk):
        ih, il = split(toks[0:64])
        base = s * 512
        rb[0:64, base : base + 256] = ih
        rb[64:128, base + 256 : base + 512] = ih
        rb[128:192, base : base + 256] = il
        rb[192:256, base + 256 : base + 512] = il
        ids = seg[:, pl.ds(pl.multiple_of(blk * nblk, nblk), nblk)]
        mask = lax.broadcasted_iota(jnp.int32, (EX, nblk), 0) == ids
        rows = toks[pl.ds(pl.multiple_of(64 + 32 * h, 32), 32)]
        for t in range(16):
            for par in range(2):
                one = jnp.where(mask, rows[2 * t + par : 2 * t + par + 1, :], 0.0)
                oh, ol = split(one)
                whi[t * 16 : t * 16 + 16, base + par * 256 : base + par * 256 + 256] = oh
                wlo[t * 16 : t * 16 + 16, base + par * 256 : base + par * 256 + 256] = ol

    def grads(s):
        cols = slice(s * 512, s * 512 + 512)
        both = dot_nt(whi[:, cols], rb[:, cols])
        return both[:, 0:128] + both[:, 128:256] + dot_nt(wlo[:, cols], rb[0:128, cols])

    weigh(0, pown, m)
    g0 = grads(0)
    px.wait_recv()
    weigh(1, ppart, partner)
    nat = (g0 + grads(1)).reshape(16, EX, 128)
    group = lax.broadcasted_iota(jnp.int32, (EX, 128), 1) // 32

    def regroup(tiles, here):
        out = None
        for g in range(4):
            moved = tiles[g] if g == here else pltpu.roll(tiles[g], 32 * ((g - here) % 4), 1)
            out = moved if out is None else jnp.where(group == g, moved, out)
        return out

    bs = []
    for b in range(2):
        for cq in range(4):
            for z in range(2):
                gbuf2[cq, b, z] = regroup([nat[8 * b + 2 * g + z] for g in range(4)], cq)
        for k in (2, 1, 3):
            to = (c + k) % 4
            n = b * 3 + k - 1
            bs.append(rc(gbuf2.at[to, b], brecv.at[k - 1, b], b_s.at[n], b_r.at[n], dp, to * 2 + h))
            launch(bs[-1])

    far = (2, 1, 3, 0)
    yy = p // 4
    xx = p % 4
    u = yy * (1 - h) + xx * h
    v = xx * (1 - h) + yy * h

    def spot(first, second):
        return (first * (4 - 3 * h) + second * (1 + 3 * h)) * 2 + zl

    def c2(b, k):
        to = (m + k) % MP
        n = b * MP + k
        return rc(fown.at[to % 2, b], fpar.at[m, b], c2_s.at[n], c2_r.at[n], dp, to)

    def near(z, k):
        src = fown.at[zl] if z == 0 else cc.at[1 - zl, u, v]
        dst = cc.at[(zl + z) % 2, u, v]
        n = 1 + z * 6 + k
        return rc(src, dst, c1_s.at[n], c1_r.at[n], spot(u, (v + k) % 4), m)

    def wide(z, k):
        row = cc.at[(zl + z) % 2, u]
        n = 4 + z * 6 + k
        return rc(row, row, c1_s.at[n], c1_r.at[n], spot((u + k) % 4, v), m)

    def c3(k):
        tp = (yy + k // 8) % 4 * 4 + (xx + k // 2 % 4) % 4
        to = tp * 2 + (zl + k % 2) % 2
        return rc(fnat.at[tp], rr.at[zl, p], c3_s.at[k], c3_r.at[k], to, m)

    def dd(k):
        ty = (yy + k // 8) % 4
        tx = (xx + k // 2 % 4) % 4
        th = (h + k % 2) % 2
        return rc(
            gb.at[ty, tx, th],
            gg.at[2 * p + h],
            dd_s.at[k],
            dd_r.at[k],
            (ty * 4 + tx) * 2 + zl,
            2 * c + th,
        )

    def own(b):
        for k in range(3):
            bs[3 * b + k].wait_recv()
        done = (gbuf2[c, b] + brecv[0, b] + brecv[1, b] + brecv[2, b]) * scale[None]
        for z in range(2):
            fown[z, b] = done[z]
        for k in (4, 5, 3, 2, 6, 7, 1):
            launch(c2(b, k))
        fpar[m, b] = fown[h, b]
        cc[zl, u, v, b] = fown[zl, b]

    def rows(b):
        for k in range(1, MP):
            c2(b, k).wait_recv()
        for q in (b, b + 2):
            for g in range(4):
                fnat[4 * q + g] = regroup([fpar[2 * cq + q // 2, b] for cq in range(4)], g)
        odd = (yy + b) % 2
        for dz in (1, 0):
            for i in (1, 0):
                for dx in far:
                    k = (2 * i + odd) * 8 + dx * 2 + dz
                    if i + dx + dz:
                        c3(k).start()
                    else:

                        @pl.when(odd == 1)
                        def _():
                            c3(k).start()

    own(0)
    own(1)
    x1 = rc(fown.at[1 - zl], cc.at[zl, u, v], c1_s.at[0], c1_r.at[0], 2 * p + 1 - zl, m)
    launch(x1)
    for k in far[:3]:
        launch(near(0, k))
    x1.wait_recv()
    for k in far[:3]:
        launch(near(1, k))
    for k in far[:3]:
        near(0, k).wait_recv()
    for k in far[:3]:
        launch(wide(0, k))
    rows(0)
    for k in far[:3]:
        near(1, k).wait_recv()
    for k in far[:3]:
        launch(wide(1, k))
    rows(1)
    sent.append(lambda: each(DP, lambda k: c3(k).wait_send()))
    rr[zl, p] = fnat[p]
    ft = rc(fnat, fnatp, ft_s, ft_r, dp, partner)
    launch(ft)

    def swap(z):
        return rc(cc.at[z], ccp.at[z], c4_s.at[z], c4_r.at[z], dp, partner)

    for z in range(2):
        for k in far[:3]:
            wide(z, k).wait_recv()
        launch(swap((zl + z) % 2))
    ft.wait_recv()
    for q in range(XY):
        feat_o[:, pl.ds(pl.multiple_of((2 * q + h) * 128, 128), 128)] = fnat[q]
        feat_o[:, pl.ds(pl.multiple_of((2 * q + 1 - h) * 128, 128), 128)] = fnatp[q]

    def turned(ref, core):
        for k in range(2):
            for z in range(2):
                tiles = []
                for y in range(4):
                    for x in range(4):
                        first = y * (1 - core) + x * core
                        second = x * (1 - core) + y * core
                        tiles.append(ref[z, first, second, k])
                hi, lo = split(jnp.concatenate(tiles, axis=0).T)
                ath[2 * core + k, :, z * 256 : z * 256 + 256] = hi
                atl[2 * core + k, :, z * 256 : z * 256 + 256] = lo

    turned(cc, h)
    swap(zl).wait_recv()
    swap(1 - zl).wait_recv()
    turned(ccp, 1 - h)
    each(DP, lambda k: c3(k).wait_recv())
    rh, rl = split(rr[...].reshape(DP * EX, 128))
    right = jnp.concatenate([rh, rl], axis=1)
    for dy in far:
        q = (yy + dy) % 4
        both = dot(ath[q], right)
        res = both[:, 0:128] + both[:, 128:256] + dot(atl[q], rh)
        gb[q] = (res * (1.0 / (DP * EX))).reshape(4, 2, 16, 128)
        for dx in far:
            for dh in (1, 0):
                if dy + dx + dh:
                    dd(dy * 8 + dx * 2 + dh).start()
    sent.append(lambda: each(DP, lambda k: dd(k).wait_send()))
    gg[2 * p + h] = gb[yy, xx, h]
    each(DP, lambda k: dd(k).wait_recv())
    for i in range(DP):
        gram_o[:, i * 128 : i * 128 + 128] = gg[i]

    drain()


def body(hidden, out_grad, proj_in, proj_out, segment_ids):
    hidden = hidden.T
    kin = hidden.shape[0]
    kout = out_grad.shape[1]
    vmem = pl.BlockSpec(memory_space=pltpu.VMEM)
    hbm = pl.BlockSpec(memory_space=pltpu.HBM)
    dma = pltpu.SemaphoreType.DMA
    scratch = [
        pltpu.VMEM(proj_in.shape, BF16),
        pltpu.VMEM(proj_out.shape, BF16),
        pltpu.VMEM(segment_ids.shape, jnp.int32),
        pltpu.VMEM((8, kin, 256), BF16),
        pltpu.VMEM((8, 256, kout), BF16),
        pltpu.VMEM((4, 128, 256), F32),
        pltpu.VMEM((4, 128, 256), F32),
        pltpu.VMEM((4, 128, 256), F32),
        pltpu.VMEM((6, 64, 256), F32),
        pltpu.VMEM((2, 64, 256), F32),
        pltpu.VMEM((128, 256), F32),
        pltpu.VMEM((128, 256), F32),
        pltpu.VMEM((256, 1024), BF16),
        pltpu.VMEM((256, 1024), BF16),
        pltpu.VMEM((256, 1024), BF16),
        pltpu.VMEM((4, 2, 2, 16, 128), F32),
        pltpu.VMEM((3, 2, 2, 16, 128), F32),
        pltpu.VMEM((2, 2, 16, 128), F32),
        pltpu.VMEM((8, 2, 16, 128), F32),
        pltpu.VMEM((16, 16, 128), F32),
        pltpu.VMEM((16, 16, 128), F32),
        pltpu.VMEM((2, 4, 4, 2, 16, 128), F32),
        pltpu.VMEM((2, 4, 4, 2, 16, 128), F32),
        pltpu.VMEM((2, 16, 16, 128), F32),
        pltpu.VMEM((4, 128, 512), BF16),
        pltpu.VMEM((4, 128, 512), BF16),
        pltpu.VMEM((4, 4, 2, 16, 128), F32),
        pltpu.VMEM((32, 16, 128), F32),
        dma((19,)),
        dma((4,)),
        dma((4,)),
        dma((6,)),
        dma((6,)),
        dma,
        dma,
        dma((6,)),
        dma((6,)),
        dma((16,)),
        dma((16,)),
        dma((16,)),
        dma((16,)),
        dma((32,)),
        dma((32,)),
        dma((2,)),
        dma((2,)),
        dma,
        dma,
        dma((32,)),
        dma((32,)),
    ]
    return pl.pallas_call(
        kernel,
        out_shape=(
            pltpu.VMEM((EX, 4096), F32),
            pltpu.VMEM((16, 4096), F32),
        ),
        in_specs=[hbm, hbm, hbm, hbm, hbm],
        out_specs=(vmem, vmem),
        scratch_shapes=scratch,
        compiler_params=pltpu.CompilerParams(
            collective_id=0, has_side_effects=True, vmem_limit_bytes=65800000
        ),
        name="projected_gram",
    )(hidden, out_grad, proj_in, proj_out, segment_ids)


def solution(mesh):
    placed = (P("dp", "mp"), P("dp", "mp"), P(None, "mp"), P(None, "mp"), P("dp", None))
    return jax.shard_map(
        body,
        mesh=mesh,
        in_specs=placed,
        out_specs=(P("dp", None), P(("dp", "mp"), None)),
        check_vma=False,
    )
```

```python
import jax
import jax.numpy as jnp
from jax import lax
from jax.experimental import pallas as pl
from jax.experimental.pallas import tpu as pltpu
from jax.sharding import PartitionSpec as P

MESH = pl.DeviceIdType.MESH
EX = 16
DP = 32
MP = 8
XY = 16
F32 = jnp.float32
BF16 = jnp.bfloat16


def split(x):
    hi = x.astype(BF16)
    return hi, (x - hi.astype(F32)).astype(BF16)


def dot_nt(a, b):
    return lax.dot_general(a, b, (((1,), (1,)), ((), ())), preferred_element_type=F32)


def dot(a, b):
    return lax.dot_general(a, b, (((1,), (0,)), ((), ())), preferred_element_type=F32)


def kernel(
    hid,
    og,
    pin_h,
    pout_h,
    seg_h,
    feat_o,
    gram_o,
    pin,
    pout,
    seg,
    hbuf,
    gbuf,
    psend,
    pmine,
    precv,
    zrecv,
    zrel,
    pown,
    ppart,
    whi,
    wlo,
    rb,
    gbuf2,
    brecv,
    fown,
    fpar,
    fnat,
    fnatp,
    cc,
    ccp,
    rr,
    ath,
    atl,
    gb,
    gg,
    lsem,
    d2d_s,
    d2d_r,
    z_s,
    z_r,
    px_s,
    px_r,
    b_s,
    b_r,
    c1_s,
    c1_r,
    c2_s,
    c2_r,
    c3_s,
    c3_r,
    c4_s,
    c4_r,
    ft_s,
    ft_r,
    dd_s,
    dd_r,
):
    dp = lax.axis_index("dp")
    m = lax.axis_index("mp")
    c = m // 2
    h = m % 2
    p = dp // 2
    zl = dp % 2
    partner = c * 2 + (1 - h)
    nblk = 256

    def rc(src, dst, ss, rs, tdp, tmp):
        return pltpu.make_async_remote_copy(
            src_ref=src,
            dst_ref=dst,
            send_sem=ss,
            recv_sem=rs,
            device_id=(tdp, tmp),
            device_id_type=MESH,
        )

    barrier = pltpu.get_barrier_semaphore()
    for k in range(1, MP):
        pl.semaphore_signal(barrier, inc=1, device_id=(dp, (m + k) % MP), device_id_type=MESH)
    sent = []

    def drain():
        for wait in sent:
            wait()

    def launch(copy):
        copy.start()
        sent.append(copy.wait_send)

    def bytes_of(ref, sem):
        return pltpu.make_async_copy(ref, ref, sem).wait

    owners = [(c + 2) % 4, (c + 1) % 4, (c + 3) % 4, c]
    blocks = []
    for o in owners:
        blocks.append(o * 2 + (1 - h))
        blocks.append(o * 2 + h)
    small = []
    for k, (src, dst) in enumerate(((pin_h, pin), (pout_h, pout), (seg_h, seg))):
        small.append(pltpu.make_async_copy(src, dst, lsem.at[16 + k]))
        small[k].start()
    loads = []
    for k, blk in enumerate(blocks):
        rows = pl.ds(pl.multiple_of(blk * nblk, nblk), nblk)
        a = pltpu.make_async_copy(hid.at[:, rows], hbuf.at[k], lsem.at[2 * k])
        b = pltpu.make_async_copy(og.at[rows], gbuf.at[k], lsem.at[2 * k + 1])
        a.start()
        b.start()
        loads.append((a, b))

    def greet_dp(k, carry):
        pl.semaphore_signal(barrier, inc=1, device_id=((dp + k) % DP, m), device_id_type=MESH)
        return carry

    lax.fori_loop(1, DP, greet_dp, 0)

    def greet_plane(k, carry):
        pl.semaphore_signal(
            barrier, inc=1, device_id=((p + k) % XY * 2 + zl, partner), device_id_type=MESH
        )
        return carry

    lax.fori_loop(1, XY, greet_plane, 0)

    rb[...] = jnp.zeros(rb.shape, BF16)

    small[2].wait()
    segv = seg[...]
    erow = lax.broadcasted_iota(jnp.int32, (EX, segv.shape[1]), 0)
    counts = jnp.sum(jnp.where(erow == segv, 1.0, 0.0).astype(F32), axis=1, keepdims=True)
    scale = 1.0 / jnp.sqrt(counts)

    small[0].wait()
    small[1].wait()

    def project(k, ref):
        loads[k][0].wait()
        ref[0:64] = dot(pin[...], hbuf[k])
        loads[k][1].wait()
        ref[64:128] = dot_nt(pout[...], gbuf[k])

    d2d = []
    zsend = []
    up = (c + 1) % 4
    down = (c + 3) % 4

    def zcopy(k, src, to):
        return rc(src, zrecv.at[k], z_s.at[k], z_r.at[k], dp, to * 2 + h)

    def finish(k):
        d2d[k].wait_recv()
        pmine[k] = pmine[k] + precv[k]
        if k == 0:
            zsend.append(zcopy(0, pmine.at[0, 0:64], down))
            zsend.append(zcopy(1, pmine.at[0, 64:128], up))
            launch(zsend[0])
            launch(zsend[1])
        if k == 1:
            zsend.append(zcopy(2, pmine.at[1, 0:64], up))
            launch(zsend[2])
        if k == 2:
            zsend.append(zcopy(3, pmine.at[2, 64:128], down))
            launch(zsend[3])

    for k in range(4):
        project(2 * k, psend.at[k])
        if k == 0:
            pl.semaphore_wait(barrier, DP - 1 + MP - 1 + XY - 1)
        d2d.append(rc(psend.at[k], precv.at[k], d2d_s.at[k], d2d_r.at[k], dp, partner))
        launch(d2d[k])
        project(2 * k + 1, pmine.at[k])
        if k >= 1:
            finish(k - 1)
    finish(3)

    zsend[0].wait_recv()
    zrel[0] = zrecv[0] + pmine[2, 0:64]
    zsend.append(zcopy(4, zrel.at[0], down))
    launch(zsend[4])
    zsend[1].wait_recv()
    zrel[1] = zrecv[1] + pmine[1, 64:128]
    zsend.append(zcopy(5, zrel.at[1], up))
    launch(zsend[5])
    zsend[2].wait_recv()
    zsend[3].wait_recv()
    zsend[4].wait_recv()
    zsend[5].wait_recv()
    pown[0:64] = pmine[3, 0:64] + zrecv[2] + zrecv[4]
    pown[64:128] = pmine[3, 64:128] + zrecv[3] + zrecv[5]

    px = rc(pown, ppart, px_s, px_r, dp, partner)
    launch(px)

    def weigh(s, toks, blk):
        ih, il = split(toks[0:64])
        base = s * 512
        rb[0:64, base : base + 256] = ih
        rb[64:128, base + 256 : base + 512] = ih
        rb[128:192, base : base + 256] = il
        rb[192:256, base + 256 : base + 512] = il
        ids = seg[:, pl.ds(pl.multiple_of(blk * nblk, nblk), nblk)]
        mask = lax.broadcasted_iota(jnp.int32, (EX, nblk), 0) == ids
        rows = toks[pl.ds(pl.multiple_of(64 + 32 * h, 32), 32)]
        for t in range(16):
            for par in range(2):
                one = jnp.where(mask, rows[2 * t + par : 2 * t + par + 1, :], 0.0)
                oh, ol = split(one)
                whi[t * 16 : t * 16 + 16, base + par * 256 : base + par * 256 + 256] = oh
                wlo[t * 16 : t * 16 + 16, base + par * 256 : base + par * 256 + 256] = ol

    def grads(s):
        cols = slice(s * 512, s * 512 + 512)
        both = dot_nt(whi[:, cols], rb[:, cols])
        return both[:, 0:128] + both[:, 128:256] + dot_nt(wlo[:, cols], rb[0:128, cols])

    weigh(0, pown, m)
    g0 = grads(0)
    px.wait_recv()
    weigh(1, ppart, partner)
    nat = (g0 + grads(1)).reshape(16, EX, 128)
    group = lax.broadcasted_iota(jnp.int32, (EX, 128), 1) // 32

    def regroup(tiles, here):
        out = None
        for g in range(4):
            moved = tiles[g] if g == here else pltpu.roll(tiles[g], 32 * ((g - here) % 4), 1)
            out = moved if out is None else jnp.where(group == g, moved, out)
        return out

    for b in range(2):
        for cq in range(4):
            for z in range(2):
                gbuf2[cq, b, z] = regroup([nat[8 * b + 2 * g + z] for g in range(4)], cq)
        for k in (2, 1, 3):
            to = (c + k) % 4
            rc(gbuf2.at[to, b], brecv.at[k - 1, b], b_s.at[b], b_r.at[b], dp, to * 2 + h).start()
        sent.append(bytes_of(brecv.at[:, b], b_s.at[b]))

    far = (2, 1, 3, 0)
    yy = p // 4
    xx = p % 4
    u = yy * (1 - h) + xx * h
    v = xx * (1 - h) + yy * h

    def spot(first, second):
        return (first * (4 - 3 * h) + second * (1 + 3 * h)) * 2 + zl

    def c2(b, k):
        to = (m + k) % MP
        return rc(fown.at[to % 2, b], fpar.at[m, b], c2_s.at[b], c2_r.at[b], dp, to)

    def near(z, k):
        src = fown.at[zl] if z == 0 else cc.at[1 - zl, u, v]
        dst = cc.at[(zl + z) % 2, u, v]
        n = 1 + z
        return rc(src, dst, c1_s.at[n], c1_r.at[n], spot(u, (v + k) % 4), m)

    def wide(z, k):
        row = cc.at[(zl + z) % 2, u]
        n = 3 + z
        return rc(row, row, c1_s.at[n], c1_r.at[n], spot((u + k) % 4, v), m)

    xs = [(xx + k) % 4 for k in range(4)]
    ys = [(yy + k) % 4 for k in range(4)]
    zs = [zl, 1 - zl]
    hs = [h, 1 - h]
    mine = zl * XY + p

    def c3(ty, tx, tz):
        tp = ty * 4 + tx
        return rc(fnat.at[tp], rr.at[mine], c3_s, c3_r, tp * 2 + tz, m)

    def dd(ty, tx, th):
        src = gb.at[ty, tx, th]
        return rc(src, gg.at[2 * p + h], dd_s, dd_r, (ty * 4 + tx) * 2 + zl, 2 * c + th)

    def own(b):
        bytes_of(brecv.at[:, b], b_r.at[b])()
        done = (gbuf2[c, b] + brecv[0, b] + brecv[1, b] + brecv[2, b]) * scale[None]
        for z in range(2):
            fown[z, b] = done[z]
        for k in (4, 5, 3, 2, 6, 7, 1):
            c2(b, k).start()
        sent.append(bytes_of(fpar.at[0:7, b], c2_s.at[b]))
        fpar[m, b] = fown[h, b]
        cc[zl, u, v, b] = fown[zl, b]

    def rows(b):
        bytes_of(fpar.at[0:7, b], c2_r.at[b])()
        for q in (b, b + 2):
            for g in range(4):
                fnat[4 * q + g] = regroup([fpar[2 * cq + q // 2, b] for cq in range(4)], g)
        odd = (yy + b) % 2
        for dz in (1, 0):
            for i in (1, 0):
                ty = (yy + 2 * i + odd) % 4
                for dx in far:
                    if i + dx + dz:
                        c3(ty, xs[dx], zs[dz]).start()
                    else:

                        @pl.when(odd == 1)
                        def _():
                            c3(ty, xs[dx], zs[dz]).start()

    own(0)
    own(1)
    x1 = rc(fown.at[1 - zl], cc.at[zl, u, v], c1_s.at[0], c1_r.at[0], 2 * p + 1 - zl, m)
    launch(x1)
    few = cc.at[0, 0, 0:3]
    many = cc.at[0, 0:3]

    def three(f, z, ref, n):
        for k in far[:3]:
            f(z, k).start()
        sent.append(bytes_of(ref, c1_s.at[n]))

    three(near, 0, few, 1)
    x1.wait_recv()
    three(near, 1, few, 2)
    bytes_of(few, c1_r.at[1])()
    three(wide, 0, many, 3)
    rows(0)
    bytes_of(few, c1_r.at[2])()
    three(wide, 1, many, 4)
    rows(1)
    sent.append(bytes_of(rr.at[0:31], c3_s))
    rr[mine] = fnat[p]
    ft = rc(fnat, fnatp, ft_s, ft_r, dp, partner)
    launch(ft)

    def swap(z):
        return rc(cc.at[z], ccp.at[z], c4_s.at[z], c4_r.at[z], dp, partner)

    for z in range(2):
        bytes_of(many, c1_r.at[3 + z])()
        launch(swap((zl + z) % 2))
    ft.wait_recv()
    for q in range(XY):
        feat_o[:, pl.ds(pl.multiple_of((2 * q + h) * 128, 128), 128)] = fnat[q]
        feat_o[:, pl.ds(pl.multiple_of((2 * q + 1 - h) * 128, 128), 128)] = fnatp[q]

    def turned(ref, core):
        for k in range(2):
            for z in range(2):
                tiles = []
                for y in range(4):
                    for x in range(4):
                        first = y * (1 - core) + x * core
                        second = x * (1 - core) + y * core
                        tiles.append(ref[z, first, second, k])
                hi, lo = split(jnp.concatenate(tiles, axis=0).T)
                ath[2 * core + k, :, z * 256 : z * 256 + 256] = hi
                atl[2 * core + k, :, z * 256 : z * 256 + 256] = lo

    turned(cc, h)
    swap(zl).wait_recv()
    swap(1 - zl).wait_recv()
    turned(ccp, 1 - h)
    bytes_of(rr.at[0:31], c3_r)()
    rh, rl = split(rr[...].reshape(DP * EX, 128))
    right = jnp.concatenate([rh, rl], axis=1)
    for dy in far:
        q = ys[dy]
        both = dot(ath[q], right)
        res = both[:, 0:128] + both[:, 128:256] + dot(atl[q], rh)
        gb[q] = (res * (1.0 / (DP * EX))).reshape(4, 2, 16, 128)
        for dx in far:
            for dh in (1, 0):
                if dy + dx + dh:
                    dd(q, xs[dx], hs[dh]).start()
    sent.append(bytes_of(gg.at[0:31], dd_s))
    gg[2 * p + h] = gb[yy, xx, h]
    bytes_of(gg.at[0:31], dd_r)()
    for i in range(DP):
        gram_o[:, i * 128 : i * 128 + 128] = gg[i]

    drain()


def body(hidden, out_grad, proj_in, proj_out, segment_ids):
    hidden = hidden.T
    kin = hidden.shape[0]
    kout = out_grad.shape[1]
    vmem = pl.BlockSpec(memory_space=pltpu.VMEM)
    hbm = pl.BlockSpec(memory_space=pltpu.HBM)
    dma = pltpu.SemaphoreType.DMA
    scratch = [
        pltpu.VMEM(proj_in.shape, BF16),
        pltpu.VMEM(proj_out.shape, BF16),
        pltpu.VMEM(segment_ids.shape, jnp.int32),
        pltpu.VMEM((8, kin, 256), BF16),
        pltpu.VMEM((8, 256, kout), BF16),
        pltpu.VMEM((4, 128, 256), F32),
        pltpu.VMEM((4, 128, 256), F32),
        pltpu.VMEM((4, 128, 256), F32),
        pltpu.VMEM((6, 64, 256), F32),
        pltpu.VMEM((2, 64, 256), F32),
        pltpu.VMEM((128, 256), F32),
        pltpu.VMEM((128, 256), F32),
        pltpu.VMEM((256, 1024), BF16),
        pltpu.VMEM((256, 1024), BF16),
        pltpu.VMEM((256, 1024), BF16),
        pltpu.VMEM((4, 2, 2, 16, 128), F32),
        pltpu.VMEM((3, 2, 2, 16, 128), F32),
        pltpu.VMEM((2, 2, 16, 128), F32),
        pltpu.VMEM((8, 2, 16, 128), F32),
        pltpu.VMEM((16, 16, 128), F32),
        pltpu.VMEM((16, 16, 128), F32),
        pltpu.VMEM((2, 4, 4, 2, 16, 128), F32),
        pltpu.VMEM((2, 4, 4, 2, 16, 128), F32),
        pltpu.VMEM((32, 16, 128), F32),
        pltpu.VMEM((4, 128, 512), BF16),
        pltpu.VMEM((4, 128, 512), BF16),
        pltpu.VMEM((4, 4, 2, 16, 128), F32),
        pltpu.VMEM((32, 16, 128), F32),
        dma((19,)),
        dma((4,)),
        dma((4,)),
        dma((6,)),
        dma((6,)),
        dma,
        dma,
        dma((2,)),
        dma((2,)),
        dma((5,)),
        dma((5,)),
        dma((2,)),
        dma((2,)),
        dma,
        dma,
        dma((2,)),
        dma((2,)),
        dma,
        dma,
        dma,
        dma,
    ]
    return pl.pallas_call(
        kernel,
        out_shape=(
            pltpu.VMEM((EX, 4096), F32),
            pltpu.VMEM((16, 4096), F32),
        ),
        in_specs=[hbm, hbm, hbm, hbm, hbm],
        out_specs=(vmem, vmem),
        scratch_shapes=scratch,
        compiler_params=pltpu.CompilerParams(
            collective_id=0, has_side_effects=True, vmem_limit_bytes=65800000
        ),
        name="projected_gram",
    )(hidden, out_grad, proj_in, proj_out, segment_ids)


def solution(mesh):
    placed = (P("dp", "mp"), P("dp", "mp"), P(None, "mp"), P(None, "mp"), P("dp", None))
    return jax.shard_map(
        body,
        mesh=mesh,
        in_specs=placed,
        out_specs=(P("dp", None), P(("dp", "mp"), None)),
        check_vma=False,
    )
```

```python
import jax
import jax.numpy as jnp
from jax import lax
from jax.experimental import pallas as pl
from jax.experimental.pallas import tpu as pltpu
from jax.sharding import PartitionSpec as P

MESH = pl.DeviceIdType.MESH
EX = 16
DP = 32
MP = 8
XY = 16
F32 = jnp.float32
BF16 = jnp.bfloat16


def split(x):
    hi = x.astype(BF16)
    return hi, (x - hi.astype(F32)).astype(BF16)


def dot_nt(a, b):
    return lax.dot_general(a, b, (((1,), (1,)), ((), ())), preferred_element_type=F32)


def dot(a, b):
    return lax.dot_general(a, b, (((1,), (0,)), ((), ())), preferred_element_type=F32)


def kernel(
    hid,
    og,
    pin_h,
    pout_h,
    seg_h,
    feat_o,
    gram_o,
    pin,
    pout,
    seg,
    hbuf,
    gbuf,
    psend,
    pmine,
    precv,
    zrecv,
    zrel,
    pown,
    ppart,
    whi,
    wlo,
    rb,
    gbuf2,
    brecv,
    fown,
    fpar,
    fnat,
    fnatp,
    cc,
    ccp,
    rr,
    ath,
    atl,
    gb,
    gg,
    lsem,
    d2d_s,
    d2d_r,
    z_s,
    z_r,
    px_s,
    px_r,
    b_s,
    b_r,
    c1_s,
    c1_r,
    c2_s,
    c2_r,
    c3_s,
    c3_r,
    c4_s,
    c4_r,
    ft_s,
    ft_r,
    dd_s,
    dd_r,
):
    dp = lax.axis_index("dp")
    m = lax.axis_index("mp")
    c = m // 2
    h = m % 2
    p = dp // 2
    zl = dp % 2
    partner = c * 2 + (1 - h)
    nblk = 256

    def rc(src, dst, ss, rs, tdp, tmp):
        return pltpu.make_async_remote_copy(
            src_ref=src,
            dst_ref=dst,
            send_sem=ss,
            recv_sem=rs,
            device_id=(tdp, tmp),
            device_id_type=MESH,
        )

    barrier = pltpu.get_barrier_semaphore()
    for k in range(1, MP):
        pl.semaphore_signal(barrier, inc=1, device_id=(dp, (m + k) % MP), device_id_type=MESH)
    sent = []

    def drain():
        for wait in sent:
            wait()

    def launch(copy):
        copy.start()
        sent.append(copy.wait_send)

    def bytes_of(ref, sem):
        return pltpu.make_async_copy(ref, ref, sem).wait

    owners = [(c + 2) % 4, (c + 1) % 4, (c + 3) % 4, c]
    blocks = []
    for o in owners:
        blocks.append(o * 2 + (1 - h))
        blocks.append(o * 2 + h)
    small = []
    for k, (src, dst) in enumerate(((pin_h, pin), (pout_h, pout), (seg_h, seg))):
        small.append(pltpu.make_async_copy(src, dst, lsem.at[16 + k]))
        small[k].start()
    loads = []
    for k, blk in enumerate(blocks):
        rows = pl.ds(pl.multiple_of(blk * nblk, nblk), nblk)
        a = pltpu.make_async_copy(hid.at[:, rows], hbuf.at[k], lsem.at[2 * k])
        b = pltpu.make_async_copy(og.at[rows], gbuf.at[k], lsem.at[2 * k + 1])
        a.start()
        b.start()
        loads.append((a, b))

    def greet_dp(k, carry):
        pl.semaphore_signal(barrier, inc=1, device_id=((dp + k) % DP, m), device_id_type=MESH)
        return carry

    lax.fori_loop(1, DP, greet_dp, 0)

    def greet_plane(k, carry):
        pl.semaphore_signal(
            barrier, inc=1, device_id=((p + k) % XY * 2 + zl, partner), device_id_type=MESH
        )
        return carry

    lax.fori_loop(1, XY, greet_plane, 0)

    rb[...] = jnp.zeros(rb.shape, BF16)

    small[2].wait()
    segv = seg[...]
    erow = lax.broadcasted_iota(jnp.int32, (EX, segv.shape[1]), 0)
    counts = jnp.sum(jnp.where(erow == segv, 1.0, 0.0).astype(F32), axis=1, keepdims=True)
    scale = 1.0 / jnp.sqrt(counts)

    small[0].wait()
    small[1].wait()

    def project(k, ref):
        loads[k][0].wait()
        ref[0:64] = dot(pin[...], hbuf[k])
        loads[k][1].wait()
        ref[64:128] = dot_nt(pout[...], gbuf[k])

    d2d = []
    zsend = []
    up = (c + 1) % 4
    down = (c + 3) % 4

    def zcopy(k, src, to):
        return rc(src, zrecv.at[k], z_s.at[k], z_r.at[k], dp, to * 2 + h)

    def finish(k):
        d2d[k].wait_recv()
        pmine[k] = pmine[k] + precv[k]
        if k == 0:
            zsend.append(zcopy(0, pmine.at[0, 0:64], down))
            zsend.append(zcopy(1, pmine.at[0, 64:128], up))
            launch(zsend[0])
            launch(zsend[1])
        if k == 1:
            zsend.append(zcopy(2, pmine.at[1, 0:64], up))
            launch(zsend[2])
        if k == 2:
            zsend.append(zcopy(3, pmine.at[2, 64:128], down))
            launch(zsend[3])

    for k in range(4):
        project(2 * k, psend.at[k])
        if k == 0:
            pl.semaphore_wait(barrier, DP - 1 + MP - 1 + XY - 1)
        d2d.append(rc(psend.at[k], precv.at[k], d2d_s.at[k], d2d_r.at[k], dp, partner))
        launch(d2d[k])
        project(2 * k + 1, pmine.at[k])
        if k >= 1:
            finish(k - 1)
    finish(3)

    zsend[0].wait_recv()
    zrel[0] = zrecv[0] + pmine[2, 0:64]
    zsend.append(zcopy(4, zrel.at[0], down))
    launch(zsend[4])
    zsend[1].wait_recv()
    zrel[1] = zrecv[1] + pmine[1, 64:128]
    zsend.append(zcopy(5, zrel.at[1], up))
    launch(zsend[5])
    px = []
    for half, (direct, relayed) in enumerate(((2, 4), (3, 5))):
        part = slice(64 * half, 64 * half + 64)
        zsend[direct].wait_recv()
        zsend[relayed].wait_recv()
        pown[part] = pmine[3, part] + zrecv[direct] + zrecv[relayed]
        px.append(rc(pown.at[part], ppart.at[part], px_s.at[half], px_r.at[half], dp, partner))
        launch(px[half])

    def weigh(s, toks, blk):
        ih, il = split(toks[0:64])
        base = s * 512
        rb[0:64, base : base + 256] = ih
        rb[64:128, base + 256 : base + 512] = ih
        rb[128:192, base : base + 256] = il
        rb[192:256, base + 256 : base + 512] = il
        ids = seg[:, pl.ds(pl.multiple_of(blk * nblk, nblk), nblk)]
        mask = lax.broadcasted_iota(jnp.int32, (EX, nblk), 0) == ids
        rows = toks[pl.ds(pl.multiple_of(64 + 32 * h, 32), 32)]
        for t in range(16):
            for par in range(2):
                one = jnp.where(mask, rows[2 * t + par : 2 * t + par + 1, :], 0.0)
                oh, ol = split(one)
                whi[t * 16 : t * 16 + 16, base + par * 256 : base + par * 256 + 256] = oh
                wlo[t * 16 : t * 16 + 16, base + par * 256 : base + par * 256 + 256] = ol

    def grads(s):
        cols = slice(s * 512, s * 512 + 512)
        both = dot_nt(whi[:, cols], rb[:, cols])
        return both[:, 0:128] + both[:, 128:256] + dot_nt(wlo[:, cols], rb[0:128, cols])

    weigh(0, pown, m)
    g0 = grads(0)
    px[0].wait_recv()
    px[1].wait_recv()
    weigh(1, ppart, partner)
    nat = (g0 + grads(1)).reshape(16, EX, 128)
    group = lax.broadcasted_iota(jnp.int32, (EX, 128), 1) // 32

    def regroup(tiles, here):
        out = None
        for g in range(4):
            moved = tiles[g] if g == here else pltpu.roll(tiles[g], 32 * ((g - here) % 4), 1)
            out = moved if out is None else jnp.where(group == g, moved, out)
        return out

    for b in range(2):
        for cq in range(4):
            for z in range(2):
                gbuf2[cq, b, z] = regroup([nat[8 * b + 2 * g + z] for g in range(4)], cq)
        for k in (2, 1, 3):
            to = (c + k) % 4
            rc(gbuf2.at[to, b], brecv.at[k - 1, b], b_s.at[b], b_r.at[b], dp, to * 2 + h).start()
        sent.append(bytes_of(brecv.at[:, b], b_s.at[b]))

    far = (2, 1, 3, 0)
    yy = p // 4
    xx = p % 4
    u = yy * (1 - h) + xx * h
    v = xx * (1 - h) + yy * h

    def spot(first, second):
        return (first * (4 - 3 * h) + second * (1 + 3 * h)) * 2 + zl

    def c2(b, k):
        to = (m + k) % MP
        return rc(fown.at[to % 2, b], fpar.at[m, b], c2_s.at[b], c2_r.at[b], dp, to)

    def near(z, k):
        src = fown.at[zl] if z == 0 else cc.at[1 - zl, u, v]
        dst = cc.at[(zl + z) % 2, u, v]
        n = 1 + z
        return rc(src, dst, c1_s.at[n], c1_r.at[n], spot(u, (v + k) % 4), m)

    def wide(z, k):
        row = cc.at[(zl + z) % 2, u]
        n = 3 + z
        return rc(row, row, c1_s.at[n], c1_r.at[n], spot((u + k) % 4, v), m)

    xs = [(xx + k) % 4 for k in range(4)]
    ys = [(yy + k) % 4 for k in range(4)]
    zs = [zl, 1 - zl]
    hs = [h, 1 - h]
    mine = zl * XY + p

    def c3(ty, tx, tz):
        tp = ty * 4 + tx
        return rc(fnat.at[tp], rr.at[mine], c3_s, c3_r, tp * 2 + tz, m)

    def dd(ty, tx, th):
        src = gb.at[ty, tx, th]
        return rc(src, gg.at[2 * p + h], dd_s, dd_r, (ty * 4 + tx) * 2 + zl, 2 * c + th)

    def own(b):
        bytes_of(brecv.at[:, b], b_r.at[b])()
        done = (gbuf2[c, b] + brecv[0, b] + brecv[1, b] + brecv[2, b]) * scale[None]
        for z in range(2):
            fown[z, b] = done[z]
        for k in (4, 5, 3, 2, 6, 7, 1):
            c2(b, k).start()
        sent.append(bytes_of(fpar.at[0:7, b], c2_s.at[b]))
        fpar[m, b] = fown[h, b]
        cc[zl, u, v, b] = fown[zl, b]

    def rows(b):
        bytes_of(fpar.at[0:7, b], c2_r.at[b])()
        for q in (b, b + 2):
            for g in range(4):
                fnat[4 * q + g] = regroup([fpar[2 * cq + q // 2, b] for cq in range(4)], g)
        odd = (yy + b) % 2
        for dz in (1, 0):
            for i in (1, 0):
                ty = (yy + 2 * i + odd) % 4
                for dx in far:
                    if i + dx + dz:
                        c3(ty, xs[dx], zs[dz]).start()
                    else:

                        @pl.when(odd == 1)
                        def _():
                            c3(ty, xs[dx], zs[dz]).start()

    own(0)
    own(1)
    x1 = rc(fown.at[1 - zl], cc.at[zl, u, v], c1_s.at[0], c1_r.at[0], 2 * p + 1 - zl, m)
    launch(x1)
    few = cc.at[0, 0, 0:3]
    many = cc.at[0, 0:3]

    def three(f, z, ref, n):
        for k in far[:3]:
            f(z, k).start()
        sent.append(bytes_of(ref, c1_s.at[n]))

    three(near, 0, few, 1)
    x1.wait_recv()
    three(near, 1, few, 2)
    bytes_of(few, c1_r.at[1])()
    three(wide, 0, many, 3)
    rows(0)
    bytes_of(few, c1_r.at[2])()
    three(wide, 1, many, 4)
    rows(1)
    sent.append(bytes_of(rr.at[0:31], c3_s))
    rr[mine] = fnat[p]
    ft = rc(fnat, fnatp, ft_s, ft_r, dp, partner)
    launch(ft)

    def swap(z):
        return rc(cc.at[z], ccp.at[z], c4_s.at[z], c4_r.at[z], dp, partner)

    for z in range(2):
        bytes_of(many, c1_r.at[3 + z])()
        launch(swap((zl + z) % 2))
    ft.wait_recv()
    for q in range(XY):
        feat_o[:, pl.ds(pl.multiple_of((2 * q + h) * 128, 128), 128)] = fnat[q]
        feat_o[:, pl.ds(pl.multiple_of((2 * q + 1 - h) * 128, 128), 128)] = fnatp[q]

    def turned(ref, core):
        for k in range(2):
            for z in range(2):
                tiles = []
                for y in range(4):
                    for x in range(4):
                        first = y * (1 - core) + x * core
                        second = x * (1 - core) + y * core
                        tiles.append(ref[z, first, second, k])
                hi, lo = split(jnp.concatenate(tiles, axis=0).T)
                ath[2 * core + k, :, z * 256 : z * 256 + 256] = hi
                atl[2 * core + k, :, z * 256 : z * 256 + 256] = lo

    turned(cc, h)
    swap(zl).wait_recv()
    swap(1 - zl).wait_recv()
    turned(ccp, 1 - h)
    bytes_of(rr.at[0:31], c3_r)()
    rh, rl = split(rr[...].reshape(DP * EX, 128))
    right = jnp.concatenate([rh, rl], axis=1)
    for dy in far:
        q = ys[dy]
        both = dot(ath[q], right)
        res = both[:, 0:128] + both[:, 128:256] + dot(atl[q], rh)
        gb[q] = (res * (1.0 / (DP * EX))).reshape(4, 2, 16, 128)
        for dx in far:
            for dh in (1, 0):
                if dy + dx + dh:
                    dd(q, xs[dx], hs[dh]).start()
    sent.append(bytes_of(gg.at[0:31], dd_s))
    gg[2 * p + h] = gb[yy, xx, h]
    bytes_of(gg.at[0:31], dd_r)()
    for i in range(DP):
        gram_o[:, i * 128 : i * 128 + 128] = gg[i]

    drain()


def store(feat, gram, feat_o, gram_o, sem):
    copies = [
        pltpu.make_async_copy(feat, feat_o, sem.at[0]),
        pltpu.make_async_copy(gram, gram_o, sem.at[1]),
    ]
    for copy in copies:
        copy.start()
    for copy in copies:
        copy.wait()


def body(hidden, out_grad, proj_in, proj_out, segment_ids):
    hidden = hidden.T
    kin = hidden.shape[0]
    kout = out_grad.shape[1]
    vmem = pl.BlockSpec(memory_space=pltpu.VMEM)
    hbm = pl.BlockSpec(memory_space=pltpu.HBM)
    dma = pltpu.SemaphoreType.DMA
    scratch = [
        pltpu.VMEM(proj_in.shape, BF16),
        pltpu.VMEM(proj_out.shape, BF16),
        pltpu.VMEM(segment_ids.shape, jnp.int32),
        pltpu.VMEM((8, kin, 256), BF16),
        pltpu.VMEM((8, 256, kout), BF16),
        pltpu.VMEM((4, 128, 256), F32),
        pltpu.VMEM((4, 128, 256), F32),
        pltpu.VMEM((4, 128, 256), F32),
        pltpu.VMEM((6, 64, 256), F32),
        pltpu.VMEM((2, 64, 256), F32),
        pltpu.VMEM((128, 256), F32),
        pltpu.VMEM((128, 256), F32),
        pltpu.VMEM((256, 1024), BF16),
        pltpu.VMEM((256, 1024), BF16),
        pltpu.VMEM((256, 1024), BF16),
        pltpu.VMEM((4, 2, 2, 16, 128), F32),
        pltpu.VMEM((3, 2, 2, 16, 128), F32),
        pltpu.VMEM((2, 2, 16, 128), F32),
        pltpu.VMEM((8, 2, 16, 128), F32),
        pltpu.VMEM((16, 16, 128), F32),
        pltpu.VMEM((16, 16, 128), F32),
        pltpu.VMEM((2, 4, 4, 2, 16, 128), F32),
        pltpu.VMEM((2, 4, 4, 2, 16, 128), F32),
        pltpu.VMEM((32, 16, 128), F32),
        pltpu.VMEM((4, 128, 512), BF16),
        pltpu.VMEM((4, 128, 512), BF16),
        pltpu.VMEM((4, 4, 2, 16, 128), F32),
        pltpu.VMEM((32, 16, 128), F32),
        dma((19,)),
        dma((4,)),
        dma((4,)),
        dma((6,)),
        dma((6,)),
        dma((2,)),
        dma((2,)),
        dma((2,)),
        dma((2,)),
        dma((5,)),
        dma((5,)),
        dma((2,)),
        dma((2,)),
        dma,
        dma,
        dma((2,)),
        dma((2,)),
        dma,
        dma,
        dma,
        dma,
    ]
    results = pl.pallas_call(
        kernel,
        out_shape=(
            pltpu.VMEM((EX, 4096), F32),
            pltpu.VMEM((16, 4096), F32),
        ),
        in_specs=[hbm, hbm, hbm, hbm, hbm],
        out_specs=(vmem, vmem),
        scratch_shapes=scratch,
        compiler_params=pltpu.CompilerParams(
            collective_id=0, has_side_effects=True, vmem_limit_bytes=65800000
        ),
        name="projected_gram",
    )(hidden, out_grad, proj_in, proj_out, segment_ids)
    return pl.pallas_call(
        store,
        out_shape=(
            jax.ShapeDtypeStruct((EX, 4096), F32),
            jax.ShapeDtypeStruct((16, 4096), F32),
        ),
        in_specs=[vmem, vmem],
        out_specs=(hbm, hbm),
        scratch_shapes=[dma((2,))],
        compiler_params=pltpu.CompilerParams(vmem_limit_bytes=1 << 20),
        name="store_results",
    )(*results)


def solution(mesh):
    placed = (P("dp", "mp"), P("dp", "mp"), P(None, "mp"), P(None, "mp"), P("dp", None))
    return jax.shard_map(
        body,
        mesh=mesh,
        in_specs=placed,
        out_specs=(P("dp", None), P(("dp", "mp"), None)),
        check_vma=False,
    )
```
